256 devices in a mesh: dp: 16 (over x, y), seq: 16 (over z, core).
Axes of the slice: x: 4, y: 4, z: 8, core: 2. Of those that a mesh axis runs over, the one named last changes fastest.
Arguments:
- tokens: bfloat16 [16, 2048, 5120], P('dp', 'seq'), may hold values from -6 to 6
- base_query: bfloat16 [16, 2048, 2560], P('dp', 'seq'), may hold values from -96 to 96
- k_base: bfloat16 [16, 2048, 2560], P('dp', 'seq'), may hold values from -4 to 4
- v_base: bfloat16 [16, 2048, 2560], P('dp', 'seq'), may hold values from -6 to 6
- cotangent: bfloat16 [16, 2048, 2560], P('dp', 'seq'), may hold values from -0.0066223145 to 0.0066223145
- adapter_down: bfloat16 [5120, 256], replicated, may hold values from -0.078125 to 0.078125
- adapter_up_weight: bfloat16 [256, 2560], replicated, may hold values from -1 to 1
- gate_weight: bfloat16 [8, 5120], replicated, may hold values from -0.078125 to 0.078125
Outputs:
- attended: bfloat16 [16, 2048, 2560], P('dp', 'seq')
- gate_grad: float32 [8, 5120], replicated
The draws below stay inside these ranges and needn't reach their ends.
All inputs are finite; a program needn't handle non-finite values.
Results may differ from the reference program's by a relative error of at most 0.03.
Values may be sent and summed in bfloat16 or wider, within the bound.
No kernel may reach another device: no remote copies, remote signals or barrier semaphores. Data moves between devices by JAX's collectives and lax.ppermute only.
A program may use at most 192 MiB of HBM per device.

```python
import jax
import jax.numpy as jnp
from jax import lax

D = 5120
HEAD_DIM = 128
HEADS = 20
EXPERTS = 8
RANK = 32
TOK_DEV = 128
LENGTH = 2048
BATCH = 16
N_DP = 16
N_SEQ = 16


def drawn_pair(key):
    shape = (BATCH, LENGTH, HEADS * HEAD_DIM)
    key_rows = jnp.clip(jax.random.normal(jax.random.fold_in(key, 7), shape, jnp.float32), -4.0, 4.0)
    query_rows = jnp.clip(jax.random.normal(jax.random.fold_in(key, 5), shape, jnp.float32), -4.0, 4.0)
    return (query_rows, key_rows)


def draw_base_query(key, part):
    return drawn_pair(key)[0].astype(jnp.bfloat16)


def draw_k_base(key, part):
    return drawn_pair(key)[1].astype(jnp.bfloat16)


def block_scale(rng, extent, split, low, top_value):
    level = 1.0
    for axis_at, shards_of in split:
        steps = jax.random.uniform(jax.random.fold_in(jax.random.fold_in(rng, 6), axis_at), (shards_of,), jnp.float32, low / len(split), top_value / len(split))
        level = level * jnp.repeat(jnp.exp(steps), extent[axis_at] // shards_of).reshape((-1,) + (1,) * (len(extent) - 1 - axis_at))
    return level


def normal_values(rng, shape, spread, limit, pieces=(), kind=jnp.bfloat16):
    values = spread * jax.random.normal(rng, shape, jnp.float32)
    if pieces:
        values = values * block_scale(rng, shape, pieces, -0.22, 0.18)
    return jnp.clip(values, -limit, limit).astype(kind)


def setup_inputs(seed: int = 0) -> dict:
    keys = jax.random.split(jax.random.key(seed), 9)
    return {
        "tokens": normal_values(keys[0], (BATCH, LENGTH, D), 1.0, 6.0, ((0, 16), (1, 16))),
        "base_query": draw_base_query(jax.random.fold_in(keys[8], 71), 0),
        "k_base": draw_k_base(jax.random.fold_in(keys[8], 71), 0),
        "v_base": normal_values(keys[3], (BATCH, LENGTH, HEADS * HEAD_DIM), 1.0, 6.0, ((0, 16), (1, 16))),
        "cotangent": normal_values(keys[4], (BATCH, LENGTH, HEADS * HEAD_DIM), (0.2 / (TOK_DEV * N_SEQ * N_DP) ** 0.5), 0.0066223145, ((0, 16), (1, 16))),
        "adapter_down": normal_values(keys[5], (D, EXPERTS * RANK), D ** -0.5, 0.078125),
        "adapter_up_weight": normal_values(keys[6], (EXPERTS * RANK, HEADS * HEAD_DIM), RANK ** -0.5, 1.0),
        "gate_weight": normal_values(keys[7], (EXPERTS, D), D ** -0.5, 0.078125),
    }


adapter_scale = 2.0
masked_score = -1e30


def reference(tokens, base_query, k_base, v_base, cotangent, adapter_down, adapter_up_weight, gate_weight):
    width = HEADS * HEAD_DIM
    score_scale = HEAD_DIM ** -0.5
    block = min(LENGTH, 256)
    block_count = LENGTH // block

    def per_sequence(inputs):
        seq_tokens, sequence_query, seq_keys, seq_values, seq_cot = inputs
        logits = jnp.dot(seq_tokens, gate_weight.T, preferred_element_type=jnp.float32)
        gates = jax.nn.softmax(logits, axis=-1)
        low = jnp.dot(seq_tokens, adapter_down, preferred_element_type=jnp.float32).astype(jnp.bfloat16)
        blended_query = (low.astype(jnp.float32) * jnp.repeat(gates, RANK, axis=1)).astype(jnp.bfloat16)
        query_matrix = (sequence_query.astype(jnp.float32) + adapter_scale * jnp.dot(blended_query, adapter_up_weight, preferred_element_type=jnp.float32)).astype(jnp.bfloat16)
        query_heads = query_matrix.reshape(LENGTH, HEADS, HEAD_DIM).astype(jnp.float32)
        key_heads = seq_keys.reshape(LENGTH, HEADS, HEAD_DIM).astype(jnp.float32)
        value_heads = seq_values.reshape(LENGTH, HEADS, HEAD_DIM).astype(jnp.float32)
        cot_heads = seq_cot.reshape(LENGTH, HEADS, HEAD_DIM).astype(jnp.float32)
        key_positions = jnp.arange(LENGTH, dtype=jnp.int32)

        def one_block(block_index):
            first_row = (block_index * block).astype(jnp.int32)
            query_rows = lax.dynamic_slice_in_dim(query_heads, first_row, block, 0)
            cot_rows = lax.dynamic_slice_in_dim(cot_heads, first_row, block, 0)
            positions = first_row + jnp.arange(block, dtype=jnp.int32)
            scores = jnp.einsum("qhd,khd->qhk", query_rows, key_heads, precision=lax.Precision.HIGHEST) * score_scale
            visible = key_positions[None, None, :] <= positions[:, None, None]
            scores = jnp.where(visible, scores, masked_score)
            probabilities = jax.nn.softmax(scores, axis=-1)
            probabilities_b = probabilities.astype(jnp.bfloat16).astype(jnp.float32)
            attended_rows = jnp.einsum("qhk,khd->qhd", probabilities_b, value_heads, precision=lax.Precision.HIGHEST)
            slopes = jnp.einsum("qhd,khd->qhk", cot_rows, value_heads, precision=lax.Precision.HIGHEST)
            products = probabilities * slopes
            delta = jnp.sum(products, axis=-1)
            scaled = products.astype(jnp.bfloat16).astype(jnp.float32)
            grad_part = jnp.einsum("qhk,khd->qhd", scaled, key_heads, precision=lax.Precision.HIGHEST)
            key_part = jnp.einsum("qhk,khd->qhd", probabilities_b, key_heads, precision=lax.Precision.HIGHEST)
            dquery_rows = score_scale * (grad_part - delta[..., None] * key_part)
            return attended_rows.astype(jnp.bfloat16), dquery_rows.astype(jnp.bfloat16)

        attended_blocks, dquery_blocks = lax.map(one_block, jnp.arange(block_count, dtype=jnp.int32))
        attended = attended_blocks.reshape(LENGTH, width)
        query_gradient = dquery_blocks.reshape(LENGTH, width)
        blended_query_gradient = adapter_scale * jnp.dot(query_gradient, adapter_up_weight.T, preferred_element_type=jnp.float32)
        dgates = (blended_query_gradient * low.astype(jnp.float32)).reshape(LENGTH, EXPERTS, RANK).sum(axis=-1)
        dlogits = gates * (dgates - jnp.sum(gates * dgates, axis=-1, keepdims=True))
        partial_grad = jnp.dot(dlogits.astype(jnp.bfloat16).T, seq_tokens, preferred_element_type=jnp.float32)
        return attended, partial_grad

    attended_all, partials = lax.map(per_sequence, (tokens, base_query, k_base, v_base, cotangent))
    return attended_all, jnp.sum(partials, axis=0)
```

```python
import functools
import math

import jax
import jax.numpy as jnp
from jax import lax
from jax.experimental import pallas as pl
from jax.experimental.pallas import tpu as pltpu
from jax.sharding import Mesh
from jax.sharding import PartitionSpec as P


HEAD_DIM = 128
EXPERTS = 8
RANK = 32
CORES = 2
AXES = ("x", "y", "z", "c")
SEQ = ("z", "c")
DP = ("x", "y")
ADAPTER_SCALE = 2.0
SCORE_SCALE = HEAD_DIM ** (-0.5)
EXP2_SCALE = SCORE_SCALE * math.log2(math.e)
MASKED = -1e30

bf16, f32 = jnp.bfloat16, jnp.float32
WHOLE = pl.BlockSpec(memory_space=pltpu.VMEM)
SCALAR = pl.BlockSpec(memory_space=pltpu.SMEM)
VMEM_LIMIT = 20 * 1024 * 1024


def rows_dot(a, b, precision=None):
    return lax.dot_general(
        a, b, (((1,), (1,)), ((), ())), precision=precision, preferred_element_type=f32
    )


def pack_body(a, b, mine, other, sems):
    half = a.shape[2] // CORES
    core = lax.axis_index("c")
    copies = []
    for out, which in ((mine, core), (other, 1 - core)):
        for at, source in ((0, a), (half, b)):
            columns = pl.ds(pl.multiple_of(which * half, HEAD_DIM), half)
            copies.append(
                pltpu.make_async_copy(
                    source.at[0, :, columns], out.at[:, pl.ds(at, half)], sems.at[len(copies)]
                )
            )
    for copy in copies:
        copy.start()
    for copy in copies:
        copy.wait()


def pack(a, b):
    _, rows, width = a.shape
    return pl.pallas_call(
        pack_body,
        in_specs=[pl.BlockSpec(memory_space=pl.ANY)] * 2,
        out_specs=[WHOLE] * 2,
        out_shape=[pltpu.VMEM((rows, width), a.dtype)] * 2,
        scratch_shapes=[pltpu.SemaphoreType.DMA((2 * CORES,))],
        name="pack",
        cost_estimate=pl.CostEstimate(flops=2_000_000, bytes_accessed=5_000_000, transcendentals=0),
    )(a, b)


def expert_columns(columns):
    e = lax.broadcasted_iota(jnp.int32, (EXPERTS, columns), 0)
    col = lax.broadcasted_iota(jnp.int32, (EXPERTS, columns), 1)
    return (col // RANK == e).astype(f32)


def query_body(tok_mine, tok_other, down, gate, up, mine, other, query, low_out, gates_out):
    rows = tok_mine.shape[0]
    half = up.shape[1]
    spread = expert_columns(down.shape[1])
    for part, tok, base in ((0, tok_mine, mine), (1, tok_other, other)):
        at = slice(part * rows, (part + 1) * rows)
        t = tok[...]
        logits = rows_dot(t, gate[...])
        e = jnp.exp(logits - jnp.max(logits, axis=-1, keepdims=True))
        gates = e / jnp.sum(e, axis=-1, keepdims=True)
        low = jnp.dot(t, down[...], preferred_element_type=f32).astype(bf16)
        wide = jnp.dot(gates, spread, precision=lax.Precision.HIGHEST, preferred_element_type=f32)
        mixed = (low.astype(f32) * wide).astype(bf16)
        product = jnp.dot(mixed, up[...], preferred_element_type=f32)
        query[at, :] = (base[:, :half].astype(f32) + ADAPTER_SCALE * product).astype(bf16)
        low_out[at, :] = low
        gates_out[at, :] = gates


def make_query(tok_mine, tok_other, down, gate, up_half, mine, other):
    rows = tok_mine.shape[0] * CORES
    half = up_half.shape[1]
    return pl.pallas_call(
        query_body,
        in_specs=[WHOLE] * 7,
        out_specs=[WHOLE] * 3,
        out_shape=[
            jax.ShapeDtypeStruct((rows, half), bf16),
            jax.ShapeDtypeStruct((rows, down.shape[1]), bf16),
            jax.ShapeDtypeStruct((rows, EXPERTS), f32),
        ],
        name="query",
        compiler_params=pltpu.CompilerParams(vmem_limit_bytes=VMEM_LIMIT),
        cost_estimate=pl.CostEstimate(
            flops=2 * rows * 256 * (5120 + half), bytes_accessed=8_000_000, transcendentals=0
        ),
    )(tok_mine, tok_other, down, gate, up_half, mine, other)


def tiled(x, width):
    return jnp.concatenate([x] * (width // x.shape[1]), axis=1)


def step(q, cot, keys, values, state, mask):
    wide = (q.shape[0], HEAD_DIM)
    scores = rows_dot(q, keys)
    if mask is not None:
        scores = jnp.where(mask, scores, MASKED)
    top = jnp.broadcast_to(jnp.max(scores, axis=-1, keepdims=True), wide)
    if state is not None:
        top = jnp.maximum(top, state[0])
        fade = jnp.exp2((state[0] - top) * EXP2_SCALE)
    weights = jnp.exp2((scores - tiled(top, scores.shape[1])) * EXP2_SCALE)
    products = weights * rows_dot(cot, values)
    total = jnp.broadcast_to(jnp.sum(weights, axis=-1, keepdims=True), wide)
    delta = jnp.broadcast_to(jnp.sum(products, axis=-1, keepdims=True), wide)
    both = jnp.dot(
        weights.astype(bf16), jnp.concatenate([values, keys], axis=1), preferred_element_type=f32
    )
    acc_v, acc_k = both[:, :HEAD_DIM], both[:, HEAD_DIM:]
    acc_g = jnp.dot(products.astype(bf16), keys, preferred_element_type=f32)
    if state is not None:
        total = total + fade * state[1]
        delta = delta + fade * state[2]
        acc_v = acc_v + fade * state[3]
        acc_k = acc_k + fade * state[4]
        acc_g = acc_g + fade * state[5]
    return top, total, delta, acc_v, acc_k, acc_g


STATES = 6


def attend_body(*refs, kind, reach, last, heads):
    refs = list(refs)
    place, token_in, query, cot_mine, other = refs[:5]
    del refs[:5]
    count = {"own": 2, "far": 4, "edge": 2}[kind]
    pieces = refs[:count]
    del refs[:count]
    state_in = None
    if kind != "own":
        state_in = refs[:STATES]
        del refs[:STATES]
    half = heads * HEAD_DIM
    rows = cot_mine.shape[0]
    both_rows = CORES * rows
    core, z = place[0], place[1]
    unroll = 2 if heads % 2 == 0 else 1

    def columns(h, base=0):
        return pl.ds(pl.multiple_of(h * HEAD_DIM + base, HEAD_DIM), HEAD_DIM)

    def head(h, piece_refs, mask=None):
        at = columns(h)
        cot = jnp.concatenate([cot_mine[:, at], other[:, columns(h, half)]], axis=0)
        keys = jnp.concatenate([p[:, at] for p in piece_refs], axis=0)
        values = jnp.concatenate([p[:, columns(h, half)] for p in piece_refs], axis=0)
        state = None if state_in is None else tuple(s[:, at] for s in state_in)
        return step(query[:, at], cot, keys, values, state, mask)

    if not last:
        token_out, state_out = refs[0], refs[1:]
        token_out[...] = jnp.zeros_like(token_out)

        def run(piece_refs, mask=None):
            def one_head(h, carry):
                new = head(h, piece_refs, mask)
                for ref, value in zip(state_out, new, strict=True):
                    ref[:, columns(h)] = value
                return carry

            lax.fori_loop(0, heads, one_head, 0, unroll=unroll)

        if kind == "own":
            shape = (both_rows, both_rows)
            r = lax.broadcasted_iota(jnp.int32, shape, 0)
            s = lax.broadcasted_iota(jnp.int32, shape, 1)
            mine_at, other_at = core * rows, (1 - core) * rows - rows
            row_at = r + jnp.where(r < rows, mine_at, other_at)
            key_at = s + jnp.where(s < rows, mine_at, other_at)
            run(pieces, key_at <= row_at)
            return
        near, wrapped = reach

        @pl.when(z >= wrapped)
        def _():
            run(pieces)

        @pl.when(jnp.logical_and(z >= near, z < wrapped))
        def _():
            run(pieces[:2])

        @pl.when(z < near)
        def _():
            for a, b in zip(state_in, state_out, strict=True):
                b[...] = a[...]

        return

    up, low, gates, tok_mine, tok_other, att_mine, att_other, grad, dmixed = refs

    def close(seen):
        def one_head(h, carry):
            at = columns(h)
            state = head(h, pieces) if seen else tuple(s[:, at] for s in state_in)
            _, total, delta, acc_v, acc_k, acc_g = state
            inverse = 1.0 / total
            attended = (acc_v * inverse).astype(bf16)
            att_mine[:, at] = attended[:rows]
            att_other[:, at] = attended[rows:]
            dquery = SCORE_SCALE * (acc_g * inverse - (delta * inverse) * (acc_k * inverse))
            dmixed[...] += rows_dot(dquery.astype(bf16), up[:, at])
            return carry

        lax.fori_loop(0, heads, one_head, 0, unroll=unroll)

    dmixed[...] = jnp.zeros_like(dmixed)
    seen = z >= reach[0]
    pl.when(seen)(lambda: close(True))
    pl.when(jnp.logical_not(seen))(lambda: close(False))
    spread = expert_columns(up.shape[0])
    dgates = rows_dot(
        ADAPTER_SCALE * dmixed[...] * low[...].astype(f32), spread, lax.Precision.HIGHEST
    )
    g = gates[...]
    dlogits = g * (dgates - jnp.sum(g * dgates, axis=-1, keepdims=True))
    turned = dlogits.T.astype(bf16)
    total = jnp.dot(turned[:, :rows], tok_mine[...], preferred_element_type=f32) + jnp.dot(
        turned[:, rows:], tok_other[...], preferred_element_type=f32
    )
    per_block = grad.shape[1] // HALF_TILE
    for i in range(grad.shape[0] * per_block):
        t, u = i // 2, i % 2
        b, j = i // per_block, i % per_block
        grad[b, j * HALF_TILE : (j + 1) * HALF_TILE, :] = total[
            u * HALF_TILE : (u + 1) * HALF_TILE, t * LANES : (t + 1) * LANES
        ]


HALF_TILE = EXPERTS // 2
LANES = 128


def gather_blocks_body(blocks, out):
    per_block = blocks.shape[1] // HALF_TILE
    for i in range(blocks.shape[0] * per_block):
        t, u = i // 2, i % 2
        b, j = i // per_block, i % per_block
        out[u * HALF_TILE : (u + 1) * HALF_TILE, t * LANES : (t + 1) * LANES] = blocks[
            b, j * HALF_TILE : (j + 1) * HALF_TILE, :
        ]


def in_vmem(x):
    return pltpu.with_memory_space_constraint(x, pltpu.VMEM)


def attend(kind, reach, place, token, query, cot_mine, other, pieces, state, tail=()):
    both_rows, half = query.shape
    heads = half // HEAD_DIM
    rows = both_rows // CORES
    last = bool(tail)
    operands = [place, token, query, cot_mine, other, *pieces, *state, *tail]
    if last:
        width = tail[-1].shape[1]
        n = lax.axis_size(SEQ)
        out_shape = [
            jax.ShapeDtypeStruct((rows, half), bf16),
            jax.ShapeDtypeStruct((rows, half), bf16),
            jax.ShapeDtypeStruct((n, EXPERTS * width // n // LANES, LANES), f32),
        ]
        scratch = [pltpu.VMEM((both_rows, tail[0].shape[0]), f32)]
    else:
        out_shape = [jax.ShapeDtypeStruct((8, LANES), f32)]
        out_shape += [pltpu.VMEM((both_rows, half), f32)] * STATES
        scratch = []
    keys = sum(p.shape[0] for p in pieces)
    return pl.pallas_call(
        functools.partial(attend_body, kind=kind, reach=reach, last=last, heads=heads),
        in_specs=[SCALAR, pl.BlockSpec(memory_space=pl.ANY)] + [WHOLE] * (len(operands) - 2),
        out_specs=[WHOLE] * len(out_shape),
        out_shape=out_shape,
        scratch_shapes=scratch,
        name="attend_" + kind,
        compiler_params=pltpu.CompilerParams(vmem_limit_bytes=VMEM_LIMIT),
        cost_estimate=pl.CostEstimate(
            flops=20 * both_rows * keys * half, bytes_accessed=8_000_000, transcendentals=0
        ),
    )(*operands)


def sent(value, axis, size):
    copies = jnp.broadcast_to(value[None], (size, *value.shape))
    return lax.all_to_all(copies, axis, 0, 0, tiled=True)


def total_of(blocks, shape):
    own = lax.all_to_all(blocks, SEQ, 0, 0, tiled=True).sum(axis=0)
    own = sent(own, DP, lax.axis_size(DP)).sum(axis=0)
    whole = sent(own, SEQ, lax.axis_size(SEQ))
    return pl.pallas_call(
        gather_blocks_body,
        in_specs=[WHOLE],
        out_specs=WHOLE,
        out_shape=jax.ShapeDtypeStruct(shape, f32),
        name="gather_blocks",
    )(whole)


def after(arrays, token):
    *arrays, token = lax.optimization_barrier((*arrays, token))
    return arrays, token


def shards(tokens, base_query, k_base, v_base, cotangent, adapter_down, up_weight, gate_weight):
    width = k_base.shape[2]
    half = width // CORES
    n = lax.axis_size("z")
    core, z = lax.axis_index("c"), lax.axis_index("z")
    place = jnp.stack([core, z]).astype(jnp.int32)
    ahead = [(i, (i + 1) % n) for i in range(n)]
    back = [(i, (i - 1) % n) for i in range(n)]
    swap = [(0, 1), (1, 0)]

    def cross(way):
        return [(2 * i + c, 2 * ((i + way) % n) + 1 - c) for i in range(n) for c in range(2)]

    a0, other_kv = pack(k_base, v_base)
    fa = [a0, lax.ppermute(a0, "z", ahead)]
    kb = [None, lax.ppermute(other_kv, SEQ, cross(-1))]
    b0 = lax.ppermute(other_kv, "c", swap)
    fb = [b0, lax.ppermute(other_kv, SEQ, cross(1))]
    ka = [a0, lax.ppermute(a0, "z", back)]
    mine_qc, other_qc = pack(base_query, cotangent)
    qc = lax.ppermute(other_qc, "c", swap)
    tok_mine = tokens[0]
    tok_other = lax.ppermute(tok_mine, "c", swap)

    up_half = lax.dynamic_slice_in_dim(up_weight, core * half, half, 1)
    query, low, gates = make_query(
        tok_mine, tok_other, adapter_down, gate_weight, up_half, mine_qc, qc
    )
    cot_mine = mine_qc[:, half:]
    common = (query, cot_mine, qc)
    fa.append(lax.ppermute(fa[1], "z", ahead))
    kb.append(lax.ppermute(kb[1], "z", back))
    token = jnp.zeros((8, LANES), f32)
    token, *state = attend("own", None, place, token, *common, (a0, b0), ())
    (x, y), token = after((fb[1], ka[1]), token)
    fb.append(lax.ppermute(x, "z", ahead))
    ka.append(lax.ppermute(y, "z", back))
    for d in range(1, n // 2):
        pieces = (fa[d], fb[d], ka[d], kb[d])
        state = [in_vmem(s) for s in state]
        token, *state = attend("far", (d, n - d), place, token, *common, pieces, state)
        if d + 1 < n // 2:
            (x, y), token = after((fa[d + 1], kb[d + 1]), token)
            fa.append(lax.ppermute(x, "z", ahead))
            kb.append(lax.ppermute(y, "z", back))
        if d + 2 < n // 2:
            fb.append(lax.ppermute(fb[d + 1], "z", ahead))
            ka.append(lax.ppermute(ka[d + 1], "z", back))
    tail = (up_half, low, gates, tok_mine, tok_other)
    state = [in_vmem(s) for s in state]
    edge = (fa[n // 2], kb[n // 2])
    att_mine, att_other, grad = attend(
        "edge", (n // 2, n), place, token, *common, edge, state, tail
    )
    att_back = lax.ppermute(att_other, "c", swap)
    attended = jnp.where(
        core == 0,
        jnp.concatenate([att_mine, att_back], axis=1),
        jnp.concatenate([att_back, att_mine], axis=1),
    )
    return attended[None], total_of(grad, (EXPERTS, tokens.shape[2]))


def solution(mesh):
    split = Mesh(mesh.devices.reshape(4, 4, 8, 2), AXES)
    rows = P(DP, SEQ, None)
    return jax.shard_map(
        shards,
        mesh=split,
        in_specs=(rows,) * 5 + (P(),) * 3,
        out_specs=(rows, P()),
        check_vma=False,
    )
```

```python
import functools
import math

import jax
import jax.numpy as jnp
from jax import lax
from jax.experimental import pallas as pl
from jax.experimental.pallas import tpu as pltpu
from jax.sharding import Mesh
from jax.sharding import PartitionSpec as P


HEAD_DIM = 128
EXPERTS = 8
RANK = 32
CORES = 2
AXES = ("x", "y", "z", "c")
SEQ = ("z", "c")
DP = ("x", "y")
ADAPTER_SCALE = 2.0
SCORE_SCALE = HEAD_DIM ** (-0.5)
EXP2_SCALE = SCORE_SCALE * math.log2(math.e)
MASKED = -1e30

bf16, f32 = jnp.bfloat16, jnp.float32
WHOLE = pl.BlockSpec(memory_space=pltpu.VMEM)
SCALAR = pl.BlockSpec(memory_space=pltpu.SMEM)
VMEM_LIMIT = 20 * 1024 * 1024


def rows_dot(a, b, precision=None):
    return lax.dot_general(
        a, b, (((1,), (1,)), ((), ())), precision=precision, preferred_element_type=f32
    )


def pack_body(a, b, mine, other, held, came, went):
    half = a.shape[2] // CORES
    core = lax.axis_index("c")
    pairs = []
    for i, (out, which) in enumerate(((mine, core), (other, 1 - core))):
        for j, source in enumerate((a, b)):
            n = len(pairs)
            columns = pl.ds(pl.multiple_of(which * half, HEAD_DIM), half)
            at = pl.ds(j * half, half)
            pairs.append(
                (
                    pltpu.make_async_copy(source.at[0, :, columns], held.at[i, :, at], came.at[n]),
                    pltpu.make_async_copy(held.at[i, :, at], out.at[:, at], went.at[n]),
                )
            )
    for come, _ in pairs:
        come.start()
    for come, go in pairs:
        come.wait()
        go.start()
    for _, go in pairs:
        go.wait()


def pack(a, b):
    _, rows, width = a.shape
    return pl.pallas_call(
        pack_body,
        in_specs=[pl.BlockSpec(memory_space=pl.ANY)] * 2,
        out_specs=[pl.BlockSpec(memory_space=pl.ANY)] * 2,
        out_shape=[pltpu.HBM((rows, width), a.dtype)] * 2,
        scratch_shapes=[
            pltpu.VMEM((CORES, rows, width), a.dtype),
            pltpu.SemaphoreType.DMA((2 * CORES,)),
            pltpu.SemaphoreType.DMA((2 * CORES,)),
        ],
        name="pack",
        cost_estimate=pl.CostEstimate(flops=2_000_000, bytes_accessed=5_000_000, transcendentals=0),
    )(a, b)


def expert_columns(columns):
    e = lax.broadcasted_iota(jnp.int32, (EXPERTS, columns), 0)
    col = lax.broadcasted_iota(jnp.int32, (EXPERTS, columns), 1)
    return (col // RANK == e).astype(f32)


def query_body(tok_mine, tok_other, down, gate, up, mine, other, query, low_out, gates_out):
    rows = tok_mine.shape[0]
    half = up.shape[1]
    spread = expert_columns(down.shape[1])
    for part, tok, base in ((0, tok_mine, mine), (1, tok_other, other)):
        at = slice(part * rows, (part + 1) * rows)
        t = tok[...]
        logits = rows_dot(t, gate[...])
        e = jnp.exp(logits - jnp.max(logits, axis=-1, keepdims=True))
        gates = e / jnp.sum(e, axis=-1, keepdims=True)
        low = jnp.dot(t, down[...], preferred_element_type=f32).astype(bf16)
        wide = jnp.dot(gates, spread, precision=lax.Precision.HIGHEST, preferred_element_type=f32)
        mixed = (low.astype(f32) * wide).astype(bf16)
        product = jnp.dot(mixed, up[...], preferred_element_type=f32)
        query[at, :] = (base[:, :half].astype(f32) + ADAPTER_SCALE * product).astype(bf16)
        low_out[at, :] = low
        gates_out[:, at] = gates.T


def make_query(tok_mine, tok_other, down, gate, up_half, mine, other):
    rows = tok_mine.shape[0] * CORES
    half = up_half.shape[1]
    return pl.pallas_call(
        query_body,
        in_specs=[WHOLE] * 7,
        out_specs=[WHOLE] * 3,
        out_shape=[
            jax.ShapeDtypeStruct((rows, half), bf16),
            jax.ShapeDtypeStruct((rows, down.shape[1]), bf16),
            jax.ShapeDtypeStruct((EXPERTS, rows), f32),
        ],
        name="query",
        compiler_params=pltpu.CompilerParams(vmem_limit_bytes=VMEM_LIMIT),
        cost_estimate=pl.CostEstimate(
            flops=2 * rows * 256 * (5120 + half), bytes_accessed=8_000_000, transcendentals=0
        ),
    )(tok_mine, tok_other, down, gate, up_half, mine, other)


def tiled(x, width):
    return jnp.concatenate([x] * (width // x.shape[1]), axis=1)


def step(q, cot, keys, values, state, mask):
    wide = (q.shape[0], HEAD_DIM)
    scores = rows_dot(q, keys)
    if mask is not None:
        scores = jnp.where(mask, scores, MASKED)
    top = jnp.broadcast_to(jnp.max(scores, axis=-1, keepdims=True), wide)
    if state is not None:
        top = jnp.maximum(top, state[0])
        fade = jnp.exp2((state[0] - top) * EXP2_SCALE)
    weights = jnp.exp2((scores - tiled(top, scores.shape[1])) * EXP2_SCALE)
    products = weights * rows_dot(cot, values)
    total = jnp.broadcast_to(jnp.sum(weights, axis=-1, keepdims=True), wide)
    delta = jnp.broadcast_to(jnp.sum(products, axis=-1, keepdims=True), wide)
    both = jnp.dot(
        weights.astype(bf16), jnp.concatenate([values, keys], axis=1), preferred_element_type=f32
    )
    acc_v, acc_k = both[:, :HEAD_DIM], both[:, HEAD_DIM:]
    acc_g = jnp.dot(products.astype(bf16), keys, preferred_element_type=f32)
    if state is not None:
        total = total + fade * state[1]
        delta = delta + fade * state[2]
        acc_v = acc_v + fade * state[3]
        acc_k = acc_k + fade * state[4]
        acc_g = acc_g + fade * state[5]
    return top, total, delta, acc_v, acc_k, acc_g


STATES = 6


def attend_body(*refs, kind, reach, last, heads):
    refs = list(refs)
    place, token_in, query, cot_mine, other = refs[:5]
    del refs[:5]
    count = {"own": 2, "far": 4, "edge": 2}[kind]
    pieces = refs[:count]
    del refs[:count]
    state_in = None
    if kind != "own":
        state_in = refs[:STATES]
        del refs[:STATES]
    half = heads * HEAD_DIM
    rows = cot_mine.shape[0]
    both_rows = CORES * rows
    core, z = place[0], place[1]
    unroll = 2 if heads % 2 == 0 else 1

    def columns(h, base=0):
        return pl.ds(pl.multiple_of(h * HEAD_DIM + base, HEAD_DIM), HEAD_DIM)

    def head(h, piece_refs, mask=None):
        at = columns(h)
        cot = jnp.concatenate([cot_mine[:, at], other[:, columns(h, half)]], axis=0)
        keys = jnp.concatenate([p[:, at] for p in piece_refs], axis=0)
        values = jnp.concatenate([p[:, columns(h, half)] for p in piece_refs], axis=0)
        state = None if state_in is None else tuple(s[:, at] for s in state_in)
        return step(query[:, at], cot, keys, values, state, mask)

    if not last:
        token_out, state_out = refs[0], refs[1:]
        token_out[...] = jnp.zeros_like(token_out)

        def run(piece_refs, mask=None):
            def one_head(h, carry):
                new = head(h, piece_refs, mask)
                for ref, value in zip(state_out, new, strict=True):
                    ref[:, columns(h)] = value
                return carry

            lax.fori_loop(0, heads, one_head, 0, unroll=unroll)

        if kind == "own":
            shape = (both_rows, both_rows)
            r = lax.broadcasted_iota(jnp.int32, shape, 0)
            s = lax.broadcasted_iota(jnp.int32, shape, 1)
            mine_at, other_at = core * rows, (1 - core) * rows - rows
            row_at = r + jnp.where(r < rows, mine_at, other_at)
            key_at = s + jnp.where(s < rows, mine_at, other_at)
            run(pieces, key_at <= row_at)
            return
        near, wrapped = reach

        @pl.when(z >= wrapped)
        def _():
            run(pieces)

        @pl.when(jnp.logical_and(z >= near, z < wrapped))
        def _():
            run(pieces[:2])

        @pl.when(z < near)
        def _():
            for a, b in zip(state_in, state_out, strict=True):
                b[...] = a[...]

        return

    up, low, gates, tok_mine, tok_other, att_mine, att_other, grad, dqueries, att, sems = refs

    def outs(at):
        return [
            pltpu.make_async_copy(att.at[pl.ds(0, rows), at], att_mine.at[:, at], sems.at[0]),
            pltpu.make_async_copy(att.at[pl.ds(rows, rows), at], att_other.at[:, at], sems.at[1]),
        ]

    def close(seen):
        def one_head(h, carry):
            at = columns(h)
            state = head(h, pieces) if seen else tuple(s[:, at] for s in state_in)
            _, total, delta, acc_v, acc_k, acc_g = state
            inverse = 1.0 / total
            att[:, at] = (acc_v * inverse).astype(bf16)
            for copy in outs(at):
                copy.start()
            dquery = SCORE_SCALE * (acc_g * inverse - (delta * inverse) * (acc_k * inverse))
            dqueries[:, at] = dquery.astype(bf16)
            return carry

        lax.fori_loop(0, heads, one_head, 0, unroll=unroll)

    seen = z >= reach[0]
    pl.when(seen)(lambda: close(True))
    pl.when(jnp.logical_not(seen))(lambda: close(False))
    spread = expert_columns(up.shape[0]).astype(bf16)
    dmixed = rows_dot(dqueries[...], up[...])
    product = ADAPTER_SCALE * dmixed * low[...].astype(f32)
    dgates = jnp.zeros((EXPERTS, both_rows), f32)
    for _ in range(3):
        part = product.astype(bf16)
        dgates = dgates + rows_dot(spread, part)
        product = product - part.astype(f32)
    g = gates[...]
    dlogits = (g * (dgates - jnp.sum(g * dgates, axis=0, keepdims=True))).astype(bf16)
    width = tok_mine.shape[1]
    chunk = CORES * LANES
    total = jnp.concatenate(
        [
            jnp.dot(
                dlogits,
                jnp.concatenate([tok_mine[:, at : at + chunk], tok_other[:, at : at + chunk]], axis=0),
                preferred_element_type=f32,
            )
            for at in range(0, width, chunk)
        ],
        axis=1,
    )
    per_block = grad.shape[1] // HALF_TILE
    for i in range(grad.shape[0] * per_block):
        t, u = i // 2, i % 2
        b, j = i // per_block, i % per_block
        grad[b, j * HALF_TILE : (j + 1) * HALF_TILE, :] = total[
            u * HALF_TILE : (u + 1) * HALF_TILE, t * LANES : (t + 1) * LANES
        ].astype(bf16)
    for copy in outs(pl.ds(0, half)):
        copy.wait()


HALF_TILE = EXPERTS // 2
LANES = 128


def gather_blocks_body(blocks, out):
    per_block = blocks.shape[1] // HALF_TILE
    for i in range(blocks.shape[0] * per_block):
        t, u = i // 2, i % 2
        b, j = i // per_block, i % per_block
        out[u * HALF_TILE : (u + 1) * HALF_TILE, t * LANES : (t + 1) * LANES] = blocks[
            b, j * HALF_TILE : (j + 1) * HALF_TILE, :
        ].astype(f32)


def in_vmem(x):
    return pltpu.with_memory_space_constraint(x, pltpu.VMEM)


def attend(kind, reach, place, token, query, cot_mine, other, pieces, state, tail=()):
    both_rows, half = query.shape
    heads = half // HEAD_DIM
    rows = both_rows // CORES
    last = bool(tail)
    operands = [place, token, query, cot_mine, other, *pieces, *state, *tail]
    if last:
        width = tail[-1].shape[1]
        n = lax.axis_size(SEQ)
        out_shape = [
            pltpu.HBM((rows, half), bf16),
            pltpu.HBM((rows, half), bf16),
            jax.ShapeDtypeStruct((n, EXPERTS * width // n // LANES, LANES), bf16),
        ]
        out_specs = [pl.BlockSpec(memory_space=pl.ANY)] * 2 + [WHOLE]
        scratch = [
            pltpu.VMEM((both_rows, half), bf16),
            pltpu.VMEM((both_rows, half), bf16),
            pltpu.SemaphoreType.DMA((CORES,)),
        ]
    else:
        out_shape = [jax.ShapeDtypeStruct((8, LANES), f32)]
        out_shape += [pltpu.VMEM((both_rows, half), f32)] * STATES
        out_specs = [WHOLE] * len(out_shape)
        scratch = []
    keys = sum(p.shape[0] for p in pieces)
    return pl.pallas_call(
        functools.partial(attend_body, kind=kind, reach=reach, last=last, heads=heads),
        in_specs=[SCALAR, pl.BlockSpec(memory_space=pl.ANY)] + [WHOLE] * (len(operands) - 2),
        out_specs=out_specs,
        out_shape=out_shape,
        scratch_shapes=scratch,
        name="attend_" + kind,
        compiler_params=pltpu.CompilerParams(vmem_limit_bytes=VMEM_LIMIT),
        cost_estimate=pl.CostEstimate(
            flops=20 * both_rows * keys * half, bytes_accessed=8_000_000, transcendentals=0
        ),
    )(*operands)


def sent(value, axis, size):
    copies = jnp.broadcast_to(value[None], (size, *value.shape))
    return lax.all_to_all(copies, axis, 0, 0, tiled=True)


def total_of(blocks, shape):
    own = lax.all_to_all(blocks, SEQ, 0, 0, tiled=True).astype(f32).sum(axis=0).astype(bf16)
    own = sent(own, DP, lax.axis_size(DP)).astype(f32).sum(axis=0).astype(bf16)
    whole = in_vmem(sent(own, SEQ, lax.axis_size(SEQ)))
    return pl.pallas_call(
        gather_blocks_body,
        in_specs=[WHOLE],
        out_specs=WHOLE,
        out_shape=jax.ShapeDtypeStruct(shape, f32),
        name="gather_blocks",
    )(whole)


def after(arrays, token):
    *arrays, token = lax.optimization_barrier((*arrays, token))
    return arrays, token


def shards(tokens, base_query, k_base, v_base, cotangent, adapter_down, up_weight, gate_weight):
    width = k_base.shape[2]
    half = width // CORES
    n = lax.axis_size("z")
    core, z = lax.axis_index("c"), lax.axis_index("z")
    place = jnp.stack([core, z]).astype(jnp.int32)
    ahead = [(i, (i + 1) % n) for i in range(n)]
    back = [(i, (i - 1) % n) for i in range(n)]
    swap = [(0, 1), (1, 0)]

    def cross(way):
        return [(2 * i + c, 2 * ((i + way) % n) + 1 - c) for i in range(n) for c in range(2)]

    a0, other_kv = pack(k_base, v_base)
    fa = [a0, lax.ppermute(a0, "z", ahead)]
    kb = [None, lax.ppermute(other_kv, SEQ, cross(-1))]
    b0 = lax.ppermute(other_kv, "c", swap)
    fb = [b0, lax.ppermute(other_kv, SEQ, cross(1))]
    ka = [a0, lax.ppermute(a0, "z", back)]
    mine_qc, other_qc = pack(base_query, cotangent)
    qc = lax.ppermute(other_qc, "c", swap)
    tok_mine = tokens[0]
    tok_other = lax.ppermute(tok_mine, "c", swap)

    up_half = lax.dynamic_slice_in_dim(up_weight, core * half, half, 1)
    query, low, gates = make_query(
        tok_mine, tok_other, adapter_down, gate_weight, up_half, mine_qc, qc
    )
    cot_mine = mine_qc[:, half:]
    common = (query, cot_mine, qc)
    fa.append(lax.ppermute(fa[1], "z", ahead))
    kb.append(lax.ppermute(kb[1], "z", back))
    token = jnp.zeros((8, LANES), f32)
    token, *state = attend("own", None, place, token, *common, (a0, b0), ())
    (x, y), token = after((fb[1], ka[1]), token)
    fb.append(lax.ppermute(x, "z", ahead))
    ka.append(lax.ppermute(y, "z", back))
    for d in range(1, n // 2):
        pieces = (fa[d], fb[d], ka[d], kb[d])
        state = [in_vmem(s) for s in state]
        token, *state = attend("far", (d, n - d), place, token, *common, pieces, state)
        if d + 1 < n // 2:
            (x, y), token = after((fa[d + 1], kb[d + 1]), token)
            fa.append(lax.ppermute(x, "z", ahead))
            kb.append(lax.ppermute(y, "z", back))
        if d + 2 < n // 2:
            fb.append(lax.ppermute(fb[d + 1], "z", ahead))
            ka.append(lax.ppermute(ka[d + 1], "z", back))
    tail = (in_vmem(up_half), low, gates, in_vmem(tok_mine), in_vmem(tok_other))
    common = tuple(in_vmem(x) for x in common)
    state = [in_vmem(s) for s in state]
    edge = (fa[n // 2], kb[n // 2])
    att_mine, att_other, grad = attend(
        "edge", (n // 2, n), place, token, *common, edge, state, tail
    )
    att_back = lax.ppermute(att_other, "c", swap)
    attended = jnp.where(
        core == 0,
        jnp.concatenate([att_mine, att_back], axis=1),
        jnp.concatenate([att_back, att_mine], axis=1),
    )
    return attended[None], total_of(grad, (EXPERTS, tokens.shape[2]))


def solution(mesh):
    split = Mesh(mesh.devices.reshape(4, 4, 8, 2), AXES)
    rows = P(DP, SEQ, None)
    return jax.shard_map(
        shards,
        mesh=split,
        in_specs=(rows,) * 5 + (P(),) * 3,
        out_specs=(rows, P()),
        check_vma=False,
    )
```

```python
import functools
import math

import jax
import jax.numpy as jnp
from jax import lax
from jax.experimental import pallas as pl
from jax.experimental.pallas import tpu as pltpu
from jax.sharding import Mesh
from jax.sharding import PartitionSpec as P


HEAD_DIM = 128
EXPERTS = 8
RANK = 32
CORES = 2
AXES = ("x", "y", "z", "c")
SEQ = ("z", "c")
DP = ("x", "y")
ADAPTER_SCALE = 2.0
SCORE_SCALE = HEAD_DIM ** (-0.5)
EXP2_SCALE = SCORE_SCALE * math.log2(math.e)
MASKED = -1e30

bf16, f32 = jnp.bfloat16, jnp.float32
WHOLE = pl.BlockSpec(memory_space=pltpu.VMEM)
SCALAR = pl.BlockSpec(memory_space=pltpu.SMEM)
VMEM_LIMIT = 20 * 1024 * 1024


def rows_dot(a, b, precision=None):
    return lax.dot_general(
        a, b, (((1,), (1,)), ((), ())), precision=precision, preferred_element_type=f32
    )


def pack_body(a, b, mine, other, held, came, went):
    half = a.shape[2] // CORES
    core = lax.axis_index("c")
    pairs = []
    for i, (out, which) in enumerate(((mine, core), (other, 1 - core))):
        for j, source in enumerate((a, b)):
            n = len(pairs)
            columns = pl.ds(pl.multiple_of(which * half, HEAD_DIM), half)
            at = pl.ds(j * half, half)
            pairs.append(
                (
                    pltpu.make_async_copy(source.at[0, :, columns], held.at[i, :, at], came.at[n]),
                    pltpu.make_async_copy(held.at[i, :, at], out.at[:, at], went.at[n]),
                )
            )
    for come, _ in pairs:
        come.start()
    for come, go in pairs:
        come.wait()
        go.start()
    for _, go in pairs:
        go.wait()


def pack(a, b):
    _, rows, width = a.shape
    return pl.pallas_call(
        pack_body,
        in_specs=[pl.BlockSpec(memory_space=pl.ANY)] * 2,
        out_specs=[pl.BlockSpec(memory_space=pl.ANY)] * 2,
        out_shape=[pltpu.HBM((rows, width), a.dtype)] * 2,
        scratch_shapes=[
            pltpu.VMEM((CORES, rows, width), a.dtype),
            pltpu.SemaphoreType.DMA((2 * CORES,)),
            pltpu.SemaphoreType.DMA((2 * CORES,)),
        ],
        name="pack",
        cost_estimate=pl.CostEstimate(flops=2_000_000, bytes_accessed=5_000_000, transcendentals=0),
    )(a, b)


def expert_columns(columns):
    e = lax.broadcasted_iota(jnp.int32, (EXPERTS, columns), 0)
    col = lax.broadcasted_iota(jnp.int32, (EXPERTS, columns), 1)
    return (col // RANK == e).astype(f32)


def query_body(tok_mine, tok_other, down, gate, up, mine, other, query, low_out, gates_out):
    rows = tok_mine.shape[0]
    half = up.shape[1]
    spread = expert_columns(down.shape[1])
    for part, tok, base in ((0, tok_mine, mine), (1, tok_other, other)):
        at = slice(part * rows, (part + 1) * rows)
        t = tok[...]
        logits = rows_dot(t, gate[...])
        e = jnp.exp(logits - jnp.max(logits, axis=-1, keepdims=True))
        gates = e / jnp.sum(e, axis=-1, keepdims=True)
        low = jnp.dot(t, down[...], preferred_element_type=f32).astype(bf16)
        wide = jnp.dot(gates, spread, precision=lax.Precision.HIGHEST, preferred_element_type=f32)
        mixed = (low.astype(f32) * wide).astype(bf16)
        product = jnp.dot(mixed, up[...], preferred_element_type=f32)
        query[at, :] = (base[:, :half].astype(f32) + ADAPTER_SCALE * product).astype(bf16)
        low_out[at, :] = low
        gates_out[:, at] = gates.T


def make_query(tok_mine, tok_other, down, gate, up_half, mine, other):
    rows = tok_mine.shape[0] * CORES
    half = up_half.shape[1]
    return pl.pallas_call(
        query_body,
        in_specs=[WHOLE] * 7,
        out_specs=[WHOLE] * 3,
        out_shape=[
            jax.ShapeDtypeStruct((rows, half), bf16),
            jax.ShapeDtypeStruct((rows, down.shape[1]), bf16),
            jax.ShapeDtypeStruct((EXPERTS, rows), f32),
        ],
        name="query",
        compiler_params=pltpu.CompilerParams(vmem_limit_bytes=VMEM_LIMIT),
        cost_estimate=pl.CostEstimate(
            flops=2 * rows * 256 * (5120 + half), bytes_accessed=8_000_000, transcendentals=0
        ),
    )(tok_mine, tok_other, down, gate, up_half, mine, other)


def tiled(x, width):
    return jnp.concatenate([x] * (width // x.shape[1]), axis=1)


def step(q, cot, keys, values, state, mask):
    wide = (q.shape[0], HEAD_DIM)
    scores = rows_dot(q, keys)
    if mask is not None:
        scores = jnp.where(mask, scores, MASKED)
    top = jnp.broadcast_to(jnp.max(scores, axis=-1, keepdims=True), wide)
    if state is not None:
        top = jnp.maximum(top, state[0])
        fade = jnp.exp2((state[0] - top) * EXP2_SCALE)
    weights = jnp.exp2((scores - tiled(top, scores.shape[1])) * EXP2_SCALE)
    products = weights * rows_dot(cot, values)
    total = jnp.broadcast_to(jnp.sum(weights, axis=-1, keepdims=True), wide)
    delta = jnp.broadcast_to(jnp.sum(products, axis=-1, keepdims=True), wide)
    both = jnp.dot(
        weights.astype(bf16), jnp.concatenate([values, keys], axis=1), preferred_element_type=f32
    )
    acc_v, acc_k = both[:, :HEAD_DIM], both[:, HEAD_DIM:]
    acc_g = jnp.dot(products.astype(bf16), keys, preferred_element_type=f32)
    if state is not None:
        total = total + fade * state[1]
        delta = delta + fade * state[2]
        acc_v = acc_v + fade * state[3]
        acc_k = acc_k + fade * state[4]
        acc_g = acc_g + fade * state[5]
    return top, total, delta, acc_v, acc_k, acc_g


STATES = 6


def attend_body(*refs, kind, reach, heads, first=0):
    refs = list(refs)
    place, _, query, cot_mine, other = refs[:5]
    del refs[:5]
    count = {"own": 2, "far": 4, "edge": 2, "close": 2}[kind]
    pieces = refs[:count]
    del refs[:count]
    state_in = None
    if kind != "own":
        state_in = refs[:STATES]
        del refs[:STATES]
    half = cot_mine.shape[1]
    rows = cot_mine.shape[0]
    both_rows = CORES * rows
    core, z = place[0], place[1]
    unroll = 2 if heads % 2 == 0 else heads

    def columns(h, base=0):
        return pl.ds(pl.multiple_of(h * HEAD_DIM + base, HEAD_DIM), HEAD_DIM)

    def head(h, piece_refs, mask=None):
        at = columns(h + first)
        cot = jnp.concatenate([cot_mine[:, at], other[:, columns(h + first, half)]], axis=0)
        keys = jnp.concatenate([p[:, columns(h)] for p in piece_refs], axis=0)
        values_at = columns(h, heads * HEAD_DIM)
        values = jnp.concatenate([p[:, values_at] for p in piece_refs], axis=0)
        state = None if state_in is None else tuple(s[:, at] for s in state_in)
        return step(query[:, at], cot, keys, values, state, mask)

    if kind in ("own", "far"):
        token_out, state_out = refs[0], refs[1:]
        token_out[...] = jnp.zeros_like(token_out)

        def run(piece_refs, mask=None):
            def one_head(h, carry):
                new = head(h, piece_refs, mask)
                for ref, value in zip(state_out, new, strict=True):
                    ref[:, columns(h)] = value
                return carry

            lax.fori_loop(0, heads, one_head, 0, unroll=unroll)

        if kind == "own":
            shape = (both_rows, both_rows)
            r = lax.broadcasted_iota(jnp.int32, shape, 0)
            s = lax.broadcasted_iota(jnp.int32, shape, 1)
            mine_at, other_at = core * rows, (1 - core) * rows - rows
            row_at = r + jnp.where(r < rows, mine_at, other_at)
            key_at = s + jnp.where(s < rows, mine_at, other_at)
            run(pieces, key_at <= row_at)
            return
        near, wrapped = reach

        @pl.when(z >= wrapped)
        def _():
            run(pieces)

        @pl.when(jnp.logical_and(z >= near, z < wrapped))
        def _():
            run(pieces[:2])

        @pl.when(z < near)
        def _():
            for a, b in zip(state_in, state_out, strict=True):
                b[...] = a[...]

        return

    if kind == "close":
        early, up, low, gates, tok_mine, tok_other = refs[:6]
        del refs[:6]
        att_mine, att_other, grad, dqueries, att, sems = refs
    else:
        att_mine, att_other, dqueries, att, sems = refs

    def outs(at):
        return [
            pltpu.make_async_copy(att.at[pl.ds(0, rows), at], att_mine.at[:, at], sems.at[0]),
            pltpu.make_async_copy(att.at[pl.ds(rows, rows), at], att_other.at[:, at], sems.at[1]),
        ]

    def close(seen):
        def one_head(h, carry):
            at = columns(h)
            state = head(h, pieces) if seen else tuple(s[:, columns(h + first)] for s in state_in)
            _, total, delta, acc_v, acc_k, acc_g = state
            inverse = 1.0 / total
            att[:, at] = (acc_v * inverse).astype(bf16)
            for copy in outs(at):
                copy.start()
            dquery = SCORE_SCALE * (acc_g * inverse - (delta * inverse) * (acc_k * inverse))
            dqueries[:, at] = dquery.astype(bf16)
            return carry

        lax.fori_loop(0, heads, one_head, 0, unroll=unroll)

    seen = z >= reach[0]
    pl.when(seen)(lambda: close(True))
    pl.when(jnp.logical_not(seen))(lambda: close(False))
    if kind == "edge":
        for copy in outs(pl.ds(0, heads * HEAD_DIM)):
            copy.wait()
        return
    split = first * HEAD_DIM
    spread = expert_columns(up.shape[0]).astype(bf16)
    dmixed = rows_dot(early[...], up[:, :split]) + rows_dot(dqueries[...], up[:, split:])
    product = ADAPTER_SCALE * dmixed * low[...].astype(f32)
    dgates = jnp.zeros((EXPERTS, both_rows), f32)
    for _ in range(3):
        part = product.astype(bf16)
        dgates = dgates + rows_dot(spread, part)
        product = product - part.astype(f32)
    g = gates[...]
    dlogits = (g * (dgates - jnp.sum(g * dgates, axis=0, keepdims=True))).astype(bf16)
    width = tok_mine.shape[1]
    chunk = CORES * LANES
    total = jnp.concatenate(
        [
            jnp.dot(
                dlogits,
                jnp.concatenate([tok_mine[:, at : at + chunk], tok_other[:, at : at + chunk]], axis=0),
                preferred_element_type=f32,
            )
            for at in range(0, width, chunk)
        ],
        axis=1,
    )
    per_block = grad.shape[1] // HALF_TILE
    for i in range(grad.shape[0] * per_block):
        t, u = i // 2, i % 2
        b, j = i // per_block, i % per_block
        grad[b, j * HALF_TILE : (j + 1) * HALF_TILE, :] = total[
            u * HALF_TILE : (u + 1) * HALF_TILE, t * LANES : (t + 1) * LANES
        ].astype(bf16)
    for copy in outs(pl.ds(0, heads * HEAD_DIM)):
        copy.wait()


HALF_TILE = EXPERTS // 2
LANES = 128


def gather_blocks_body(blocks, out):
    per_block = blocks.shape[1] // HALF_TILE
    for i in range(blocks.shape[0] * per_block):
        t, u = i // 2, i % 2
        b, j = i // per_block, i % per_block
        out[u * HALF_TILE : (u + 1) * HALF_TILE, t * LANES : (t + 1) * LANES] = blocks[
            b, j * HALF_TILE : (j + 1) * HALF_TILE, :
        ].astype(f32)


def in_vmem(x):
    return pltpu.with_memory_space_constraint(x, pltpu.VMEM)


def attend(kind, reach, place, token, query, cot_mine, other, pieces, state, tail=()):
    both_rows, half = query.shape
    heads = pieces[0].shape[1] // (2 * HEAD_DIM)
    rows = both_rows // CORES
    here = heads * HEAD_DIM
    first = 0
    operands = [place, token, query, cot_mine, other, *pieces, *state, *tail]
    if kind in ("own", "far"):
        out_shape = [jax.ShapeDtypeStruct((8, LANES), f32)]
        out_shape += [pltpu.VMEM((both_rows, half), f32)] * STATES
        out_specs = [WHOLE] * len(out_shape)
        scratch = []
    else:
        out_shape = [pltpu.HBM((rows, here), bf16)] * CORES
        scratch = [pltpu.VMEM((both_rows, here), bf16), pltpu.SemaphoreType.DMA((CORES,))]
        if kind == "edge":
            out_shape += [pltpu.VMEM((both_rows, here), bf16)]
        else:
            first = tail[0].shape[1] // HEAD_DIM
            n, width = lax.axis_size(SEQ), tail[-1].shape[1]
            blocks = (n, EXPERTS * width // n // LANES, LANES)
            out_shape += [jax.ShapeDtypeStruct(blocks, bf16)]
            scratch = [pltpu.VMEM((both_rows, here), bf16)] + scratch
        out_specs = [pl.BlockSpec(memory_space=pl.ANY)] * CORES + [WHOLE]
    keys = sum(p.shape[0] for p in pieces)
    return pl.pallas_call(
        functools.partial(attend_body, kind=kind, reach=reach, heads=heads, first=first),
        in_specs=[SCALAR, pl.BlockSpec(memory_space=pl.ANY)] + [WHOLE] * (len(operands) - 2),
        out_specs=out_specs,
        out_shape=out_shape,
        scratch_shapes=scratch,
        compiler_params=pltpu.CompilerParams(vmem_limit_bytes=VMEM_LIMIT),
        cost_estimate=pl.CostEstimate(
            flops=20 * both_rows * keys * here, bytes_accessed=8_000_000, transcendentals=0
        ),
    )(*operands)


def sent(value, axis, size):
    copies = jnp.broadcast_to(value[None], (size, *value.shape))
    return lax.all_to_all(copies, axis, 0, 0, tiled=True)


def total_of(blocks, shape):
    own = lax.all_to_all(blocks, SEQ, 0, 0, tiled=True).astype(f32).sum(axis=0).astype(bf16)
    own = sent(own, DP, lax.axis_size(DP)).astype(f32).sum(axis=0).astype(bf16)
    whole = in_vmem(sent(own, SEQ, lax.axis_size(SEQ)))
    return pl.pallas_call(
        gather_blocks_body,
        in_specs=[WHOLE],
        out_specs=WHOLE,
        out_shape=jax.ShapeDtypeStruct(shape, f32),
        name="gather_blocks",
    )(whole)


def after(arrays, token):
    *arrays, token = lax.optimization_barrier((*arrays, token))
    return arrays, token


def shards(tokens, base_query, k_base, v_base, cotangent, adapter_down, up_weight, gate_weight):
    width = k_base.shape[2]
    half = width // CORES
    n = lax.axis_size("z")
    core, z = lax.axis_index("c"), lax.axis_index("z")
    place = jnp.stack([core, z]).astype(jnp.int32)
    ahead = [(i, (i + 1) % n) for i in range(n)]
    back = [(i, (i - 1) % n) for i in range(n)]
    swap = [(0, 1), (1, 0)]

    def cross(way):
        return [(2 * i + c, 2 * ((i + way) % n) + 1 - c) for i in range(n) for c in range(2)]

    a0, other_kv = pack(k_base, v_base)
    fa = [a0, lax.ppermute(a0, "z", ahead)]
    kb = [None, lax.ppermute(other_kv, SEQ, cross(-1))]
    b0 = lax.ppermute(other_kv, "c", swap)
    fb = [b0, lax.ppermute(other_kv, SEQ, cross(1))]
    ka = [a0, lax.ppermute(a0, "z", back)]
    mine_qc, other_qc = pack(base_query, cotangent)
    qc = lax.ppermute(other_qc, "c", swap)
    tok_mine = tokens[0]
    tok_other = lax.ppermute(tok_mine, "c", swap)

    up_half = lax.dynamic_slice_in_dim(up_weight, core * half, half, 1)
    query, low, gates = make_query(
        tok_mine, tok_other, adapter_down, gate_weight, up_half, mine_qc, qc
    )
    cot_mine = mine_qc[:, half:]
    common = (query, cot_mine, qc)
    fa.append(lax.ppermute(fa[1], "z", ahead))
    kb.append(lax.ppermute(kb[1], "z", back))
    token = jnp.zeros((8, LANES), f32)
    token, *state = attend("own", None, place, token, *common, (a0, b0), ())
    (x, y), token = after((fb[1], ka[1]), token)
    fb.append(lax.ppermute(x, "z", ahead))
    ka.append(lax.ppermute(y, "z", back))
    for d in range(1, n // 2):
        pieces = (fa[d], fb[d], ka[d], kb[d])
        state = [in_vmem(s) for s in state]
        token, *state = attend("far", (d, n - d), place, token, *common, pieces, state)
        if d + 1 < n // 2:
            (x, y), token = after((fa[d + 1], kb[d + 1]), token)
            if d + 2 < n // 2:
                fa.append(lax.ppermute(x, "z", ahead))
                kb.append(lax.ppermute(y, "z", back))
        if d + 2 < n // 2:
            fb.append(moved(fb[d + 1], ahead))
            ka.append(moved(ka[d + 1], back))
    parts = []
    for j in range(2):
        cut = [head_part(p, j) for p in (x, y)]
        parts.append((moved(cut[0], ahead), moved(cut[1], back)))
    common = tuple(in_vmem(v) for v in common)
    state = [in_vmem(v) for v in state]
    reach = (n // 2, n)
    mine_1, other_1, early = attend("edge", reach, place, token, *common, parts[0], state)
    tail = (in_vmem(early), in_vmem(up_half), low, gates, in_vmem(tok_mine), in_vmem(tok_other))
    mine_2, other_2, grad = attend("close", reach, place, token, *common, parts[1], state, tail)
    back_1, back_2 = lax.ppermute(other_1, "c", swap), lax.ppermute(other_2, "c", swap)
    attended = jnp.where(
        core == 0,
        jnp.concatenate([mine_1, mine_2, back_1, back_2], axis=1),
        jnp.concatenate([back_1, back_2, mine_1, mine_2], axis=1),
    )
    return attended[None], total_of(grad, (EXPERTS, tokens.shape[2]))


def moved(value, pairs):
    return lax.ppermute(value, "z", pairs)


def head_part(piece, j):
    width = piece.shape[1] // 4
    keys = piece[:, j * width : (j + 1) * width]
    values = piece[:, (2 + j) * width : (3 + j) * width]
    return jnp.concatenate([keys, values], axis=1)


def solution(mesh):
    split = Mesh(mesh.devices.reshape(4, 4, 8, 2), AXES)
    rows = P(DP, SEQ, None)
    return jax.shard_map(
        shards,
        mesh=split,
        in_specs=(rows,) * 5 + (P(),) * 3,
        out_specs=(rows, P()),
        check_vma=False,
    )
```

```python
import functools
import math

import jax
import jax.numpy as jnp
from jax import lax
from jax.experimental import pallas as pl
from jax.experimental.pallas import tpu as pltpu
from jax.sharding import Mesh
from jax.sharding import PartitionSpec as P


HEAD_DIM = 128
EXPERTS = 8
RANK = 32
CORES = 2
AXES = ("x", "y", "z", "c")
SEQ = ("z", "c")
DP = ("x", "y")
ADAPTER_SCALE = 2.0
SCORE_SCALE = HEAD_DIM ** (-0.5)
EXP2_SCALE = SCORE_SCALE * math.log2(math.e)
MASKED = -1e30

bf16, f32 = jnp.bfloat16, jnp.float32
WHOLE = pl.BlockSpec(memory_space=pltpu.VMEM)
SCALAR = pl.BlockSpec(memory_space=pltpu.SMEM)
VMEM_LIMIT = 20 * 1024 * 1024


def rows_dot(a, b, precision=None):
    return lax.dot_general(
        a, b, (((1,), (1,)), ((), ())), precision=precision, preferred_element_type=f32
    )


def pack_body(a, b, mine, other, held, came, went):
    half = a.shape[2] // CORES
    core = lax.axis_index("c")
    pairs = []
    for i, (out, which) in enumerate(((mine, core), (other, 1 - core))):
        for j, source in enumerate((a, b)):
            n = len(pairs)
            columns = pl.ds(pl.multiple_of(which * half, HEAD_DIM), half)
            at = pl.ds(j * half, half)
            pairs.append(
                (
                    pltpu.make_async_copy(source.at[0, :, columns], held.at[i, :, at], came.at[n]),
                    pltpu.make_async_copy(held.at[i, :, at], out.at[:, at], went.at[n]),
                )
            )
    for come, _ in pairs:
        come.start()
    for come, go in pairs:
        come.wait()
        go.start()
    for _, go in pairs:
        go.wait()


def pack(a, b):
    _, rows, width = a.shape
    return pl.pallas_call(
        pack_body,
        in_specs=[pl.BlockSpec(memory_space=pl.ANY)] * 2,
        out_specs=[pl.BlockSpec(memory_space=pl.ANY)] * 2,
        out_shape=[pltpu.HBM((rows, width), a.dtype)] * 2,
        scratch_shapes=[
            pltpu.VMEM((CORES, rows, width), a.dtype),
            pltpu.SemaphoreType.DMA((2 * CORES,)),
            pltpu.SemaphoreType.DMA((2 * CORES,)),
        ],
        name="pack",
        cost_estimate=pl.CostEstimate(flops=2_000_000, bytes_accessed=5_000_000, transcendentals=0),
    )(a, b)


def expert_columns(columns):
    e = lax.broadcasted_iota(jnp.int32, (EXPERTS, columns), 0)
    col = lax.broadcasted_iota(jnp.int32, (EXPERTS, columns), 1)
    return (col // RANK == e).astype(f32)


def query_body(
    tok_mine, tok_other, down, gate, up, mine, other, query, low_out, gates_out, tok_kept
):
    rows = tok_mine.shape[0]
    tok_kept[...] = tok_other[...]
    half = up.shape[1]
    spread = expert_columns(down.shape[1])
    for part, tok, base in ((0, tok_mine, mine), (1, tok_other, other)):
        at = slice(part * rows, (part + 1) * rows)
        t = tok[...]
        logits = rows_dot(t, gate[...])
        e = jnp.exp(logits - jnp.max(logits, axis=-1, keepdims=True))
        gates = e / jnp.sum(e, axis=-1, keepdims=True)
        low = jnp.dot(t, down[...], preferred_element_type=f32).astype(bf16)
        wide = jnp.dot(gates, spread, precision=lax.Precision.HIGHEST, preferred_element_type=f32)
        mixed = (low.astype(f32) * wide).astype(bf16)
        product = jnp.dot(mixed, up[...], preferred_element_type=f32)
        query[at, :] = (base[:, :half].astype(f32) + ADAPTER_SCALE * product).astype(bf16)
        low_out[at, :] = low
        gates_out[:, at] = gates.T


def make_query(tok_mine, tok_other, down, gate, up_half, mine, other):
    rows = tok_mine.shape[0] * CORES
    half = up_half.shape[1]
    return pl.pallas_call(
        query_body,
        in_specs=[WHOLE] * 7,
        out_specs=[WHOLE] * 4,
        out_shape=[
            jax.ShapeDtypeStruct((rows, half), bf16),
            jax.ShapeDtypeStruct((rows, down.shape[1]), bf16),
            jax.ShapeDtypeStruct((EXPERTS, rows), f32),
            pltpu.VMEM(tok_other.shape, tok_other.dtype),
        ],
        name="query",
        compiler_params=pltpu.CompilerParams(vmem_limit_bytes=VMEM_LIMIT),
        cost_estimate=pl.CostEstimate(
            flops=2 * rows * 256 * (5120 + half), bytes_accessed=8_000_000, transcendentals=0
        ),
    )(tok_mine, tok_other, down, gate, up_half, mine, other)


def tiled(x, width):
    return jnp.concatenate([x] * (width // x.shape[1]), axis=1)


def step(q, cot, keys, values, state, mask):
    wide = (q.shape[0], HEAD_DIM)
    scores = rows_dot(q, keys)
    if mask is not None:
        scores = jnp.where(mask, scores, MASKED)
    top = jnp.broadcast_to(jnp.max(scores, axis=-1, keepdims=True), wide)
    if state is not None:
        top = jnp.maximum(top, state[0])
        fade = jnp.exp2((state[0] - top) * EXP2_SCALE)
    weights = jnp.exp2((scores - tiled(top, scores.shape[1])) * EXP2_SCALE)
    products = weights * rows_dot(cot, values)
    total = jnp.broadcast_to(jnp.sum(weights, axis=-1, keepdims=True), wide)
    delta = jnp.broadcast_to(jnp.sum(products, axis=-1, keepdims=True), wide)
    both = jnp.dot(
        weights.astype(bf16), jnp.concatenate([values, keys], axis=1), preferred_element_type=f32
    )
    acc_v, acc_k = both[:, :HEAD_DIM], both[:, HEAD_DIM:]
    acc_g = jnp.dot(products.astype(bf16), keys, preferred_element_type=f32)
    if state is not None:
        total = total + fade * state[1]
        delta = delta + fade * state[2]
        acc_v = acc_v + fade * state[3]
        acc_k = acc_k + fade * state[4]
        acc_g = acc_g + fade * state[5]
    return top, total, delta, acc_v, acc_k, acc_g


STATES = 6


def attend_body(*refs, kind, reach, heads, first=0):
    refs = list(refs)
    place, _, query, cot_mine, other = refs[:5]
    del refs[:5]
    count = {"own": 2, "far": 4, "edge": 2, "close": 2}[kind]
    pieces = refs[:count]
    del refs[:count]
    state_in = None
    if kind != "own":
        state_in = refs[:STATES]
        del refs[:STATES]
    half = cot_mine.shape[1]
    rows = cot_mine.shape[0]
    both_rows = CORES * rows
    core, z = place[0], place[1]
    unroll = 2 if heads % 2 == 0 else heads

    def columns(h, base=0):
        return pl.ds(pl.multiple_of(h * HEAD_DIM + base, HEAD_DIM), HEAD_DIM)

    def head(h, piece_refs, mask=None):
        at = columns(h + first)
        cot = jnp.concatenate([cot_mine[:, at], other[:, columns(h + first, half)]], axis=0)
        keys = jnp.concatenate([p[:, columns(h)] for p in piece_refs], axis=0)
        values_at = columns(h, heads * HEAD_DIM)
        values = jnp.concatenate([p[:, values_at] for p in piece_refs], axis=0)
        state = None if state_in is None else tuple(s[:, at] for s in state_in)
        return step(query[:, at], cot, keys, values, state, mask)

    if kind in ("own", "far"):
        token_out, state_out = refs[0], refs[1:]
        token_out[...] = jnp.zeros_like(token_out)

        def run(piece_refs, mask=None):
            def one_head(h, carry):
                new = head(h, piece_refs, mask)
                for ref, value in zip(state_out, new, strict=True):
                    ref[:, columns(h)] = value
                return carry

            lax.fori_loop(0, heads, one_head, 0, unroll=unroll)

        if kind == "own":
            shape = (both_rows, both_rows)
            r = lax.broadcasted_iota(jnp.int32, shape, 0)
            s = lax.broadcasted_iota(jnp.int32, shape, 1)
            mine_at, other_at = core * rows, (1 - core) * rows - rows
            row_at = r + jnp.where(r < rows, mine_at, other_at)
            key_at = s + jnp.where(s < rows, mine_at, other_at)
            run(pieces, key_at <= row_at)
            return
        near, wrapped = reach

        @pl.when(z >= wrapped)
        def _():
            run(pieces)

        @pl.when(jnp.logical_and(z >= near, z < wrapped))
        def _():
            run(pieces[:2])

        @pl.when(z < near)
        def _():
            for a, b in zip(state_in, state_out, strict=True):
                b[...] = a[...]

        return

    if kind == "close":
        early, up, low, gates, tok_mine, tok_other = refs[:6]
        del refs[:6]
        att_mine, att_other, grad, dqueries, att, sems = refs
    else:
        att_mine, att_other, dqueries, att, sems = refs

    def outs(at):
        return [
            pltpu.make_async_copy(att.at[pl.ds(0, rows), at], att_mine.at[:, at], sems.at[0]),
            pltpu.make_async_copy(att.at[pl.ds(rows, rows), at], att_other.at[:, at], sems.at[1]),
        ]

    def close(seen):
        def one_head(h, carry):
            at = columns(h)
            state = head(h, pieces) if seen else tuple(s[:, columns(h + first)] for s in state_in)
            _, total, delta, acc_v, acc_k, acc_g = state
            inverse = 1.0 / total
            att[:, at] = (acc_v * inverse).astype(bf16)
            for copy in outs(at):
                copy.start()
            dquery = SCORE_SCALE * (acc_g * inverse - (delta * inverse) * (acc_k * inverse))
            dqueries[:, at] = dquery.astype(bf16)
            return carry

        lax.fori_loop(0, heads, one_head, 0, unroll=unroll)

    seen = z >= reach[0]
    pl.when(seen)(lambda: close(True))
    pl.when(jnp.logical_not(seen))(lambda: close(False))
    if kind == "edge":
        for copy in outs(pl.ds(0, heads * HEAD_DIM)):
            copy.wait()
        return
    split = first * HEAD_DIM
    spread = expert_columns(up.shape[0]).astype(bf16)
    dmixed = rows_dot(early[...], up[:, :split]) + rows_dot(dqueries[...], up[:, split:])
    product = ADAPTER_SCALE * dmixed * low[...].astype(f32)
    dgates = jnp.zeros((EXPERTS, both_rows), f32)
    for _ in range(3):
        part = product.astype(bf16)
        dgates = dgates + rows_dot(spread, part)
        product = product - part.astype(f32)
    g = gates[...]
    dlogits = (g * (dgates - jnp.sum(g * dgates, axis=0, keepdims=True))).astype(bf16)
    width = tok_mine.shape[1]
    chunk = CORES * LANES
    total = jnp.concatenate(
        [
            jnp.dot(
                dlogits,
                jnp.concatenate([tok_mine[:, at : at + chunk], tok_other[:, at : at + chunk]], axis=0),
                preferred_element_type=f32,
            )
            for at in range(0, width, chunk)
        ],
        axis=1,
    )
    per_block = grad.shape[1] // HALF_TILE
    for i in range(grad.shape[0] * per_block):
        t, u = i // 2, i % 2
        b, j = i // per_block, i % per_block
        grad[b, j * HALF_TILE : (j + 1) * HALF_TILE, :] = total[
            u * HALF_TILE : (u + 1) * HALF_TILE, t * LANES : (t + 1) * LANES
        ].astype(bf16)
    for copy in outs(pl.ds(0, heads * HEAD_DIM)):
        copy.wait()


HALF_TILE = EXPERTS // 2
LANES = 128


def gather_blocks_body(blocks, out):
    per_block = blocks.shape[1] // HALF_TILE
    for i in range(blocks.shape[0] * per_block):
        t, u = i // 2, i % 2
        b, j = i // per_block, i % per_block
        out[u * HALF_TILE : (u + 1) * HALF_TILE, t * LANES : (t + 1) * LANES] = blocks[
            b, j * HALF_TILE : (j + 1) * HALF_TILE, :
        ].astype(f32)


def in_vmem(x):
    return pltpu.with_memory_space_constraint(x, pltpu.VMEM)


def attend(kind, reach, place, token, query, cot_mine, other, pieces, state, tail=()):
    both_rows, half = query.shape
    heads = pieces[0].shape[1] // (2 * HEAD_DIM)
    rows = both_rows // CORES
    here = heads * HEAD_DIM
    first = 0
    operands = [place, token, query, cot_mine, other, *pieces, *state, *tail]
    if kind in ("own", "far"):
        out_shape = [jax.ShapeDtypeStruct((8, LANES), f32)]
        out_shape += [pltpu.VMEM((both_rows, half), f32)] * STATES
        out_specs = [WHOLE] * len(out_shape)
        scratch = []
    else:
        out_shape = [pltpu.HBM((rows, here), bf16)] * CORES
        scratch = [pltpu.VMEM((both_rows, here), bf16), pltpu.SemaphoreType.DMA((CORES,))]
        if kind == "edge":
            out_shape += [pltpu.VMEM((both_rows, here), bf16)]
        else:
            first = tail[0].shape[1] // HEAD_DIM
            n, width = lax.axis_size(SEQ), tail[-1].shape[1]
            blocks = (n, EXPERTS * width // n // LANES, LANES)
            out_shape += [jax.ShapeDtypeStruct(blocks, bf16)]
            scratch = [pltpu.VMEM((both_rows, here), bf16)] + scratch
        out_specs = [pl.BlockSpec(memory_space=pl.ANY)] * CORES + [WHOLE]
    keys = sum(p.shape[0] for p in pieces)
    return pl.pallas_call(
        functools.partial(attend_body, kind=kind, reach=reach, heads=heads, first=first),
        in_specs=[SCALAR, pl.BlockSpec(memory_space=pl.ANY)] + [WHOLE] * (len(operands) - 2),
        out_specs=out_specs,
        out_shape=out_shape,
        scratch_shapes=scratch,
        compiler_params=pltpu.CompilerParams(vmem_limit_bytes=VMEM_LIMIT),
        cost_estimate=pl.CostEstimate(
            flops=20 * both_rows * keys * here, bytes_accessed=8_000_000, transcendentals=0
        ),
    )(*operands)


def sent(value, axis, size):
    copies = jnp.broadcast_to(value[None], (size, *value.shape))
    return lax.all_to_all(copies, axis, 0, 0, tiled=True)


def total_of(blocks, shape):
    own = lax.all_to_all(blocks, SEQ, 0, 0, tiled=True).astype(f32).sum(axis=0).astype(bf16)
    own = sent(own, DP, lax.axis_size(DP)).astype(f32).sum(axis=0).astype(bf16)
    whole = in_vmem(sent(own, SEQ, lax.axis_size(SEQ)))
    return pl.pallas_call(
        gather_blocks_body,
        in_specs=[WHOLE],
        out_specs=WHOLE,
        out_shape=jax.ShapeDtypeStruct(shape, f32),
        name="gather_blocks",
    )(whole)


def after(arrays, token):
    *arrays, token = lax.optimization_barrier((*arrays, token))
    return arrays, token


def shards(tokens, base_query, k_base, v_base, cotangent, adapter_down, up_weight, gate_weight):
    width = k_base.shape[2]
    half = width // CORES
    n = lax.axis_size("z")
    core, z = lax.axis_index("c"), lax.axis_index("z")
    place = jnp.stack([core, z]).astype(jnp.int32)
    ahead = [(i, (i + 1) % n) for i in range(n)]
    back = [(i, (i - 1) % n) for i in range(n)]
    swap = [(0, 1), (1, 0)]

    def cross(way):
        return [(2 * i + c, 2 * ((i + way) % n) + 1 - c) for i in range(n) for c in range(2)]

    a0, other_kv = pack(k_base, v_base)
    fa = [a0, moved(a0, ahead)]
    kb = [None, moved(other_kv, cross(-1), SEQ)]
    b0 = lax.ppermute(other_kv, "c", swap)
    fb = [b0, lax.ppermute(other_kv, SEQ, cross(1))]
    ka = [a0, lax.ppermute(a0, "z", back)]
    mine_qc, other_qc = pack(base_query, cotangent)
    qc = lax.ppermute(other_qc, "c", swap)
    tok_mine = tokens[0]
    tok_other = moved(tok_mine, swap, "c")

    up_half = lax.dynamic_slice_in_dim(up_weight, core * half, half, 1)
    query, low, gates, tok_other = make_query(
        tok_mine, tok_other, adapter_down, gate_weight, up_half, mine_qc, qc
    )
    cot_mine = mine_qc[:, half:]
    common = (query, cot_mine, qc)
    fa.append(lax.ppermute(fa[1], "z", ahead))
    kb.append(lax.ppermute(kb[1], "z", back))
    token = jnp.zeros((8, LANES), f32)
    token, *state = attend("own", None, place, token, *common, (a0, b0), ())
    (x, y), token = after((fb[1], ka[1]), token)
    fb.append(lax.ppermute(x, "z", ahead))
    ka.append(lax.ppermute(y, "z", back))
    for d in range(1, n // 2):
        pieces = (fa[d], fb[d], ka[d], kb[d])
        state = [in_vmem(s) for s in state]
        token, *state = attend("far", (d, n - d), place, token, *common, pieces, state)
        if d + 1 < n // 2:
            (x, y), token = after((fa[d + 1], kb[d + 1]), token)
            if d + 2 < n // 2:
                fa.append(lax.ppermute(x, "z", ahead))
                kb.append(lax.ppermute(y, "z", back))
        if d + 2 < n // 2:
            fb.append(moved(fb[d + 1], ahead))
            ka.append(moved(ka[d + 1], back))
    parts = []
    heads = half // HEAD_DIM
    split = heads // 2 + heads % 4 // 2
    for start, stop in ((0, split), (split, heads)):
        cut = [head_part(p, start, stop) for p in (x, y)]
        parts.append((moved(cut[0], ahead), moved(cut[1], back)))
    common = tuple(in_vmem(v) for v in common)
    state = [in_vmem(v) for v in state]
    reach = (n // 2, n)
    mine_1, other_1, early = attend("edge", reach, place, token, *common, parts[0], state)
    tail = (in_vmem(early), in_vmem(up_half), low, gates, in_vmem(tok_mine), in_vmem(tok_other))
    mine_2, other_2, grad = attend("close", reach, place, token, *common, parts[1], state, tail)
    back_1, back_2 = lax.ppermute(other_1, "c", swap), lax.ppermute(other_2, "c", swap)
    attended = jnp.where(
        core == 0,
        jnp.concatenate([mine_1, mine_2, back_1, back_2], axis=1),
        jnp.concatenate([back_1, back_2, mine_1, mine_2], axis=1),
    )
    return attended[None], total_of(grad, (EXPERTS, tokens.shape[2]))


def moved(value, pairs, axis="z"):
    return lax.ppermute(value, axis, pairs)


def head_part(piece, start, stop):
    half = piece.shape[1] // 2
    a, b = start * HEAD_DIM, stop * HEAD_DIM
    return jnp.concatenate([piece[:, a:b], piece[:, half + a : half + b]], axis=1)


def solution(mesh):
    split = Mesh(mesh.devices.reshape(4, 4, 8, 2), AXES)
    rows = P(DP, SEQ, None)
    return jax.shard_map(
        shards,
        mesh=split,
        in_specs=(rows,) * 5 + (P(),) * 3,
        out_specs=(rows, P()),
        check_vma=False,
    )
```

```python
import functools
import math

import jax
import jax.numpy as jnp
from jax import lax
from jax.experimental import pallas as pl
from jax.experimental.pallas import tpu as pltpu
from jax.sharding import Mesh
from jax.sharding import PartitionSpec as P


HEAD_DIM = 128
EXPERTS = 8
RANK = 32
CORES = 2
AXES = ("x", "y", "z", "c")
SEQ = ("z", "c")
DP = ("x", "y")
ADAPTER_SCALE = 2.0
SCORE_SCALE = HEAD_DIM ** (-0.5)
EXP2_SCALE = SCORE_SCALE * math.log2(math.e)
MASKED = -1e30

bf16, f32 = jnp.bfloat16, jnp.float32
WHOLE = pl.BlockSpec(memory_space=pltpu.VMEM)
SCALAR = pl.BlockSpec(memory_space=pltpu.SMEM)
VMEM_LIMIT = 20 * 1024 * 1024


def rows_dot(a, b, precision=None):
    return lax.dot_general(
        a, b, (((1,), (1,)), ((), ())), precision=precision, preferred_element_type=f32
    )


def pack_body(a, b, mine, other, held, came, went):
    half = a.shape[2] // CORES
    core = lax.axis_index("c")
    pairs = []
    for i, (out, which) in enumerate(((mine, core), (other, 1 - core))):
        for j, source in enumerate((a, b)):
            n = len(pairs)
            columns = pl.ds(pl.multiple_of(which * half, HEAD_DIM), half)
            at = pl.ds(j * half, half)
            pairs.append(
                (
                    pltpu.make_async_copy(source.at[0, :, columns], held.at[i, :, at], came.at[n]),
                    pltpu.make_async_copy(held.at[i, :, at], out.at[:, at], went.at[n]),
                )
            )
    for come, _ in pairs:
        come.start()
    for come, go in pairs:
        come.wait()
        go.start()
    for _, go in pairs:
        go.wait()


def pack(a, b):
    _, rows, width = a.shape
    return pl.pallas_call(
        pack_body,
        in_specs=[pl.BlockSpec(memory_space=pl.ANY)] * 2,
        out_specs=[pl.BlockSpec(memory_space=pl.ANY)] * 2,
        out_shape=[pltpu.HBM((rows, width), a.dtype)] * 2,
        scratch_shapes=[
            pltpu.VMEM((CORES, rows, width), a.dtype),
            pltpu.SemaphoreType.DMA((2 * CORES,)),
            pltpu.SemaphoreType.DMA((2 * CORES,)),
        ],
        name="pack",
        cost_estimate=pl.CostEstimate(flops=2_000_000, bytes_accessed=5_000_000, transcendentals=0),
    )(a, b)


def expert_columns(columns):
    e = lax.broadcasted_iota(jnp.int32, (EXPERTS, columns), 0)
    col = lax.broadcasted_iota(jnp.int32, (EXPERTS, columns), 1)
    return (col // RANK == e).astype(f32)


def query_body(
    tok_mine, tok_other, down, gate, up, mine, other, query, low_out, gates_out, tok_kept
):
    rows = tok_mine.shape[0]
    tok_kept[...] = tok_other[...]
    half = up.shape[1]
    spread = expert_columns(down.shape[1])
    for part, tok, base in ((0, tok_mine, mine), (1, tok_other, other)):
        at = slice(part * rows, (part + 1) * rows)
        t = tok[...]
        logits = rows_dot(t, gate[...])
        e = jnp.exp(logits - jnp.max(logits, axis=-1, keepdims=True))
        gates = e / jnp.sum(e, axis=-1, keepdims=True)
        low = jnp.dot(t, down[...], preferred_element_type=f32).astype(bf16)
        wide = jnp.dot(gates, spread, precision=lax.Precision.HIGHEST, preferred_element_type=f32)
        mixed = (low.astype(f32) * wide).astype(bf16)
        product = jnp.dot(mixed, up[...], preferred_element_type=f32)
        query[at, :] = (base[:, :half].astype(f32) + ADAPTER_SCALE * product).astype(bf16)
        low_out[at, :] = low
        gates_out[:, at] = gates.T


def make_query(tok_mine, tok_other, down, gate, up_half, mine, other):
    rows = tok_mine.shape[0] * CORES
    half = up_half.shape[1]
    return pl.pallas_call(
        query_body,
        in_specs=[WHOLE] * 7,
        out_specs=[WHOLE] * 4,
        out_shape=[
            jax.ShapeDtypeStruct((rows, half), bf16),
            jax.ShapeDtypeStruct((rows, down.shape[1]), bf16),
            jax.ShapeDtypeStruct((EXPERTS, rows), f32),
            pltpu.VMEM(tok_other.shape, tok_other.dtype),
        ],
        name="query",
        compiler_params=pltpu.CompilerParams(vmem_limit_bytes=VMEM_LIMIT),
        cost_estimate=pl.CostEstimate(
            flops=2 * rows * 256 * (5120 + half), bytes_accessed=8_000_000, transcendentals=0
        ),
    )(tok_mine, tok_other, down, gate, up_half, mine, other)


def tiled(x, width):
    return jnp.concatenate([x] * (width // x.shape[1]), axis=1)


def step(q, cot, keys, values, state, mask):
    wide = (q.shape[0], HEAD_DIM)
    scores = rows_dot(q, keys)
    if mask is not None:
        scores = jnp.where(mask, scores, MASKED)
    top = jnp.broadcast_to(jnp.max(scores, axis=-1, keepdims=True), wide)
    if state is not None:
        top = jnp.maximum(top, state[0])
        fade = jnp.exp2((state[0] - top) * EXP2_SCALE)
    weights = jnp.exp2((scores - tiled(top, scores.shape[1])) * EXP2_SCALE)
    products = weights * rows_dot(cot, values)
    total = jnp.broadcast_to(jnp.sum(weights, axis=-1, keepdims=True), wide)
    delta = jnp.broadcast_to(jnp.sum(products, axis=-1, keepdims=True), wide)
    both = jnp.dot(
        weights.astype(bf16), jnp.concatenate([values, keys], axis=1), preferred_element_type=f32
    )
    acc_v, acc_k = both[:, :HEAD_DIM], both[:, HEAD_DIM:]
    acc_g = jnp.dot(products.astype(bf16), keys, preferred_element_type=f32)
    if state is not None:
        total = total + fade * state[1]
        delta = delta + fade * state[2]
        acc_v = acc_v + fade * state[3]
        acc_k = acc_k + fade * state[4]
        acc_g = acc_g + fade * state[5]
    return top, total, delta, acc_v, acc_k, acc_g


STATES = 6


def attend_body(*refs, kind, reach, heads, first=0):
    refs = list(refs)
    place, _, query, cot_mine, other = refs[:5]
    del refs[:5]
    count = {"own": 2, "far": 4, "edge": 2, "close": 2}[kind]
    pieces = refs[:count]
    del refs[:count]
    state_in = None
    if kind != "own":
        state_in = refs[:STATES]
        del refs[:STATES]
    half = cot_mine.shape[1]
    rows = cot_mine.shape[0]
    both_rows = CORES * rows
    core, z = place[0], place[1]
    unroll = 2 if heads % 2 == 0 else heads

    def columns(h, base=0):
        return pl.ds(pl.multiple_of(h * HEAD_DIM + base, HEAD_DIM), HEAD_DIM)

    def head(h, piece_refs, mask=None):
        at = columns(h + first)
        cot = jnp.concatenate([cot_mine[:, at], other[:, columns(h + first, half)]], axis=0)
        keys = jnp.concatenate([p[:, columns(h)] for p in piece_refs], axis=0)
        values_at = columns(h, heads * HEAD_DIM)
        values = jnp.concatenate([p[:, values_at] for p in piece_refs], axis=0)
        state = None if state_in is None else tuple(s[:, at] for s in state_in)
        return step(query[:, at], cot, keys, values, state, mask)

    if kind in ("own", "far"):
        token_out, state_out = refs[0], refs[1:]
        token_out[...] = jnp.zeros_like(token_out)

        def run(piece_refs, mask=None):
            def one_head(h, carry):
                new = head(h, piece_refs, mask)
                for ref, value in zip(state_out, new, strict=True):
                    ref[:, columns(h)] = value
                return carry

            lax.fori_loop(0, heads, one_head, 0, unroll=unroll)

        if kind == "own":
            shape = (both_rows, both_rows)
            r = lax.broadcasted_iota(jnp.int32, shape, 0)
            s = lax.broadcasted_iota(jnp.int32, shape, 1)
            mine_at, other_at = core * rows, (1 - core) * rows - rows
            row_at = r + jnp.where(r < rows, mine_at, other_at)
            key_at = s + jnp.where(s < rows, mine_at, other_at)
            run(pieces, key_at <= row_at)
            return
        near, wrapped = reach

        @pl.when(z >= wrapped)
        def _():
            run(pieces)

        @pl.when(jnp.logical_and(z >= near, z < wrapped))
        def _():
            run(pieces[:2])

        @pl.when(z < near)
        def _():
            for a, b in zip(state_in, state_out, strict=True):
                b[...] = a[...]

        return

    if kind == "close":
        early, up, low, gates, tok_mine, tok_other = refs[:6]
        del refs[:6]
        att_mine, att_other, grad, dqueries, att, sems = refs
    else:
        att_mine, att_other, dqueries, att, sems = refs

    def outs(at):
        return [
            pltpu.make_async_copy(att.at[pl.ds(0, rows), at], att_mine.at[:, at], sems.at[0]),
            pltpu.make_async_copy(att.at[pl.ds(rows, rows), at], att_other.at[:, at], sems.at[1]),
        ]

    def close(seen):
        def one_head(h, carry):
            at = columns(h)
            state = head(h, pieces) if seen else tuple(s[:, columns(h + first)] for s in state_in)
            _, total, delta, acc_v, acc_k, acc_g = state
            inverse = 1.0 / total
            att[:, at] = (acc_v * inverse).astype(bf16)
            for copy in outs(at):
                copy.start()
            dquery = SCORE_SCALE * (acc_g * inverse - (delta * inverse) * (acc_k * inverse))
            dqueries[:, at] = dquery.astype(bf16)
            return carry

        lax.fori_loop(0, heads, one_head, 0, unroll=unroll)

    seen = z >= reach[0]
    pl.when(seen)(lambda: close(True))
    pl.when(jnp.logical_not(seen))(lambda: close(False))
    if kind == "edge":
        for copy in outs(pl.ds(0, heads * HEAD_DIM)):
            copy.wait()
        return
    split = first * HEAD_DIM
    spread = expert_columns(up.shape[0]).astype(bf16)
    dmixed = rows_dot(early[...], up[:, :split]) + rows_dot(dqueries[...], up[:, split:])
    product = ADAPTER_SCALE * dmixed * low[...].astype(f32)
    dgates = jnp.zeros((EXPERTS, both_rows), f32)
    for _ in range(3):
        part = product.astype(bf16)
        dgates = dgates + rows_dot(spread, part)
        product = product - part.astype(f32)
    g = gates[...]
    dlogits = (g * (dgates - jnp.sum(g * dgates, axis=0, keepdims=True))).astype(bf16)
    width = tok_mine.shape[1]
    chunk = CORES * LANES
    total = jnp.concatenate(
        [
            jnp.dot(
                dlogits,
                jnp.concatenate([tok_mine[:, at : at + chunk], tok_other[:, at : at + chunk]], axis=0),
                preferred_element_type=f32,
            )
            for at in range(0, width, chunk)
        ],
        axis=1,
    )
    per_block = grad.shape[1] // HALF_TILE
    for i in range(grad.shape[0] * per_block):
        t, u = i // 2, i % 2
        b, j = i // per_block, i % per_block
        grad[b, j * HALF_TILE : (j + 1) * HALF_TILE, :] = total[
            u * HALF_TILE : (u + 1) * HALF_TILE, t * LANES : (t + 1) * LANES
        ].astype(bf16)
    for copy in outs(pl.ds(0, heads * HEAD_DIM)):
        copy.wait()


HALF_TILE = EXPERTS // 2
LANES = 128


def gather_blocks_body(blocks, out):
    per_block = blocks.shape[1] // HALF_TILE
    for i in range(blocks.shape[0] * per_block):
        t, u = i // 2, i % 2
        b, j = i // per_block, i % per_block
        out[u * HALF_TILE : (u + 1) * HALF_TILE, t * LANES : (t + 1) * LANES] = blocks[
            b, j * HALF_TILE : (j + 1) * HALF_TILE, :
        ].astype(f32)


def in_vmem(x):
    return pltpu.with_memory_space_constraint(x, pltpu.VMEM)


def attend(kind, reach, place, token, query, cot_mine, other, pieces, state, tail=()):
    both_rows, half = query.shape
    heads = pieces[0].shape[1] // (2 * HEAD_DIM)
    rows = both_rows // CORES
    here = heads * HEAD_DIM
    first = 0
    operands = [place, token, query, cot_mine, other, *pieces, *state, *tail]
    if kind in ("own", "far"):
        out_shape = [jax.ShapeDtypeStruct((8, LANES), f32)]
        out_shape += [pltpu.VMEM((both_rows, half), f32)] * STATES
        out_specs = [WHOLE] * len(out_shape)
        scratch = []
    else:
        out_shape = [pltpu.HBM((rows, here), bf16)] * CORES
        scratch = [pltpu.VMEM((both_rows, here), bf16), pltpu.SemaphoreType.DMA((CORES,))]
        if kind == "edge":
            out_shape += [pltpu.VMEM((both_rows, here), bf16)]
        else:
            first = tail[0].shape[1] // HEAD_DIM
            n, width = lax.axis_size(SEQ), tail[-1].shape[1]
            blocks = (n, EXPERTS * width // n // LANES, LANES)
            out_shape += [jax.ShapeDtypeStruct(blocks, bf16)]
            scratch = [pltpu.VMEM((both_rows, here), bf16)] + scratch
        out_specs = [pl.BlockSpec(memory_space=pl.ANY)] * CORES + [WHOLE]
    keys = sum(p.shape[0] for p in pieces)
    return pl.pallas_call(
        functools.partial(attend_body, kind=kind, reach=reach, heads=heads, first=first),
        in_specs=[SCALAR, pl.BlockSpec(memory_space=pl.ANY)] + [WHOLE] * (len(operands) - 2),
        out_specs=out_specs,
        out_shape=out_shape,
        scratch_shapes=scratch,
        compiler_params=pltpu.CompilerParams(vmem_limit_bytes=VMEM_LIMIT),
        cost_estimate=pl.CostEstimate(
            flops=20 * both_rows * keys * here, bytes_accessed=8_000_000, transcendentals=0
        ),
    )(*operands)


def sent(value, axis, size):
    copies = jnp.broadcast_to(value[None], (size, *value.shape))
    return lax.all_to_all(copies, axis, 0, 0, tiled=True)


def total_of(blocks, shape):
    own = lax.all_to_all(blocks, SEQ, 0, 0, tiled=True).astype(f32).sum(axis=0).astype(bf16)
    own = sent(own, DP, lax.axis_size(DP)).astype(f32).sum(axis=0).astype(bf16)
    whole = in_vmem(sent(own, SEQ, lax.axis_size(SEQ)))
    return pl.pallas_call(
        gather_blocks_body,
        in_specs=[WHOLE],
        out_specs=WHOLE,
        out_shape=jax.ShapeDtypeStruct(shape, f32),
        name="gather_blocks",
    )(whole)


def after(arrays, token):
    *arrays, token = lax.optimization_barrier((*arrays, token))
    return arrays, token


def shards(tokens, base_query, k_base, v_base, cotangent, adapter_down, up_weight, gate_weight):
    width = k_base.shape[2]
    half = width // CORES
    n = lax.axis_size("z")
    core, z = lax.axis_index("c"), lax.axis_index("z")
    place = jnp.stack([core, z]).astype(jnp.int32)
    ahead = [(i, (i + 1) % n) for i in range(n)]
    back = [(i, (i - 1) % n) for i in range(n)]
    swap = [(0, 1), (1, 0)]

    def cross(way):
        return [(2 * i + c, 2 * ((i + way) % n) + 1 - c) for i in range(n) for c in range(2)]

    def halves(x):
        return [lax.dynamic_slice_in_dim(x[0], w * half, half, 1) for w in (core, 1 - core)]

    k_mine, k_other = halves(k_base)
    fa = [moved(k_mine, ahead)]
    kb = [moved(k_other, cross(-1), SEQ)]
    v_mine, v_other = halves(v_base)
    fa = [None, jnp.concatenate([fa[0], moved(v_mine, ahead)], axis=1)]
    v_back = moved(v_other, cross(-1), SEQ)
    kb = [None, jnp.concatenate([kb[0], v_back], axis=1)]
    a0 = jnp.concatenate([k_mine, v_mine], axis=1)
    other_kv = jnp.concatenate([k_other, v_other], axis=1)
    b0 = moved(other_kv, swap, "c")
    fb = [b0, moved(other_kv, cross(1), SEQ)]
    ka = [a0, moved(a0, back)]
    mine_qc, other_qc = pack(base_query, cotangent)
    qc = moved(other_qc, swap, "c")
    tok_mine = tokens[0]
    tok_other = moved(tok_mine, swap, "c")

    up_half = lax.dynamic_slice_in_dim(up_weight, core * half, half, 1)
    query, low, gates, tok_other = make_query(
        tok_mine, tok_other, adapter_down, gate_weight, up_half, mine_qc, qc
    )
    cot_mine = mine_qc[:, half:]
    common = (query, cot_mine, qc)
    fa.append(lax.ppermute(fa[1], "z", ahead))
    kb.append(lax.ppermute(kb[1], "z", back))
    token = jnp.zeros((8, LANES), f32)
    token, *state = attend("own", None, place, token, *common, (a0, b0), ())
    (x, y), token = after((fb[1], ka[1]), token)
    fb.append(lax.ppermute(x, "z", ahead))
    ka.append(lax.ppermute(y, "z", back))
    for d in range(1, n // 2):
        pieces = (fa[d], fb[d], ka[d], kb[d])
        state = [in_vmem(s) for s in state]
        token, *state = attend("far", (d, n - d), place, token, *common, pieces, state)
        if d + 1 < n // 2:
            (x, y), token = after((fa[d + 1], kb[d + 1]), token)
            if d + 2 < n // 2:
                fa.append(lax.ppermute(x, "z", ahead))
                kb.append(lax.ppermute(y, "z", back))
        if d + 2 < n // 2:
            fb.append(moved(fb[d + 1], ahead))
            ka.append(moved(ka[d + 1], back))
    parts = []
    heads = half // HEAD_DIM
    split = heads // 2 + heads % 4 // 2
    for start, stop in ((0, split), (split, heads)):
        cut = [head_part(p, start, stop) for p in (x, y)]
        parts.append((moved(cut[0], ahead), moved(cut[1], back)))
    common = tuple(in_vmem(v) for v in common)
    state = [in_vmem(v) for v in state]
    reach = (n // 2, n)
    mine_1, other_1, early = attend("edge", reach, place, token, *common, parts[0], state)
    tail = (in_vmem(early), in_vmem(up_half), low, gates, in_vmem(tok_mine), in_vmem(tok_other))
    mine_2, other_2, grad = attend("close", reach, place, token, *common, parts[1], state, tail)
    back_1, back_2 = lax.ppermute(other_1, "c", swap), lax.ppermute(other_2, "c", swap)
    attended = jnp.where(
        core == 0,
        jnp.concatenate([mine_1, mine_2, back_1, back_2], axis=1),
        jnp.concatenate([back_1, back_2, mine_1, mine_2], axis=1),
    )
    return attended[None], total_of(grad, (EXPERTS, tokens.shape[2]))


def moved(value, pairs, axis="z"):
    return lax.ppermute(value, axis, pairs)


def head_part(piece, start, stop):
    half = piece.shape[1] // 2
    a, b = start * HEAD_DIM, stop * HEAD_DIM
    return jnp.concatenate([piece[:, a:b], piece[:, half + a : half + b]], axis=1)


def solution(mesh):
    split = Mesh(mesh.devices.reshape(4, 4, 8, 2), AXES)
    rows = P(DP, SEQ, None)
    return jax.shard_map(
        shards,
        mesh=split,
        in_specs=(rows,) * 5 + (P(),) * 3,
        out_specs=(rows, P()),
        check_vma=False,
    )
```

```python
import functools
import math

import jax
import jax.numpy as jnp
from jax import lax
from jax.experimental import pallas as pl
from jax.experimental.pallas import tpu as pltpu
from jax.sharding import Mesh
from jax.sharding import PartitionSpec as P


HEAD_DIM = 128
EXPERTS = 8
RANK = 32
CORES = 2
AXES = ("x", "y", "z", "c")
SEQ = ("z", "c")
DP = ("x", "y")
ADAPTER_SCALE = 2.0
SCORE_SCALE = HEAD_DIM ** (-0.5)
EXP2_SCALE = SCORE_SCALE * math.log2(math.e)
MASKED = -1e30

bf16, f32 = jnp.bfloat16, jnp.float32
WHOLE = pl.BlockSpec(memory_space=pltpu.VMEM)
SCALAR = pl.BlockSpec(memory_space=pltpu.SMEM)
VMEM_LIMIT = 20 * 1024 * 1024


def rows_dot(a, b, precision=None):
    return lax.dot_general(
        a, b, (((1,), (1,)), ((), ())), precision=precision, preferred_element_type=f32
    )


def halve_body(a, mine, other, held, came, went):
    half = a.shape[2] // CORES
    core = lax.axis_index("c")
    pairs = []
    for i, (out, which) in enumerate(((mine, core), (other, 1 - core))):
        columns = pl.ds(pl.multiple_of(which * half, HEAD_DIM), half)
        pairs.append(
            (
                pltpu.make_async_copy(a.at[0, :, columns], held.at[i], came.at[i]),
                pltpu.make_async_copy(held.at[i], out, went.at[i]),
            )
        )
    for come, _ in pairs:
        come.start()
    for come, go in pairs:
        come.wait()
        go.start()
    for _, go in pairs:
        go.wait()


def halve(a):
    _, rows, width = a.shape
    half = width // CORES
    return pl.pallas_call(
        halve_body,
        in_specs=[pl.BlockSpec(memory_space=pl.ANY)],
        out_specs=[pl.BlockSpec(memory_space=pl.ANY)] * 2,
        out_shape=[pltpu.HBM((rows, half), a.dtype)] * 2,
        scratch_shapes=[
            pltpu.VMEM((CORES, rows, half), a.dtype),
            pltpu.SemaphoreType.DMA((CORES,)),
            pltpu.SemaphoreType.DMA((CORES,)),
        ],
        name="halve",
        cost_estimate=pl.CostEstimate(flops=1_000_000, bytes_accessed=2_600_000, transcendentals=0),
    )(a)


def pack_body(a, b, mine, other, held, came, went):
    half = a.shape[2] // CORES
    core = lax.axis_index("c")
    pairs = []
    for i, (out, which) in enumerate(((mine, core), (other, 1 - core))):
        for j, source in enumerate((a, b)):
            n = len(pairs)
            columns = pl.ds(pl.multiple_of(which * half, HEAD_DIM), half)
            at = pl.ds(j * half, half)
            pairs.append(
                (
                    pltpu.make_async_copy(source.at[0, :, columns], held.at[i, :, at], came.at[n]),
                    pltpu.make_async_copy(held.at[i, :, at], out.at[:, at], went.at[n]),
                )
            )
    for come, _ in pairs:
        come.start()
    for come, go in pairs:
        come.wait()
        go.start()
    for _, go in pairs:
        go.wait()


def pack(a, b):
    _, rows, width = a.shape
    return pl.pallas_call(
        pack_body,
        in_specs=[pl.BlockSpec(memory_space=pl.ANY)] * 2,
        out_specs=[pl.BlockSpec(memory_space=pl.ANY)] * 2,
        out_shape=[pltpu.HBM((rows, width), a.dtype)] * 2,
        scratch_shapes=[
            pltpu.VMEM((CORES, rows, width), a.dtype),
            pltpu.SemaphoreType.DMA((2 * CORES,)),
            pltpu.SemaphoreType.DMA((2 * CORES,)),
        ],
        name="pack",
        cost_estimate=pl.CostEstimate(flops=2_000_000, bytes_accessed=5_000_000, transcendentals=0),
    )(a, b)


def expert_columns(columns):
    e = lax.broadcasted_iota(jnp.int32, (EXPERTS, columns), 0)
    col = lax.broadcasted_iota(jnp.int32, (EXPERTS, columns), 1)
    return (col // RANK == e).astype(f32)


def query_body(
    tok_mine, tok_other, down, gate, up, mine, other, query, low_out, gates_out, tok_kept
):
    rows = tok_mine.shape[0]
    tok_kept[...] = tok_other[...]
    half = up.shape[1]
    spread = expert_columns(down.shape[1])
    for part, tok, base in ((0, tok_mine, mine), (1, tok_other, other)):
        at = slice(part * rows, (part + 1) * rows)
        t = tok[...]
        logits = rows_dot(t, gate[...])
        e = jnp.exp(logits - jnp.max(logits, axis=-1, keepdims=True))
        gates = e / jnp.sum(e, axis=-1, keepdims=True)
        low = jnp.dot(t, down[...], preferred_element_type=f32).astype(bf16)
        wide = jnp.dot(gates, spread, precision=lax.Precision.HIGHEST, preferred_element_type=f32)
        mixed = (low.astype(f32) * wide).astype(bf16)
        product = jnp.dot(mixed, up[...], preferred_element_type=f32)
        query[at, :] = (base[:, :half].astype(f32) + ADAPTER_SCALE * product).astype(bf16)
        low_out[at, :] = low
        gates_out[:, at] = gates.T


def make_query(tok_mine, tok_other, down, gate, up_half, mine, other):
    rows = tok_mine.shape[0] * CORES
    half = up_half.shape[1]
    return pl.pallas_call(
        query_body,
        in_specs=[WHOLE] * 7,
        out_specs=[WHOLE] * 4,
        out_shape=[
            jax.ShapeDtypeStruct((rows, half), bf16),
            jax.ShapeDtypeStruct((rows, down.shape[1]), bf16),
            jax.ShapeDtypeStruct((EXPERTS, rows), f32),
            pltpu.VMEM(tok_other.shape, tok_other.dtype),
        ],
        name="query",
        compiler_params=pltpu.CompilerParams(vmem_limit_bytes=VMEM_LIMIT),
        cost_estimate=pl.CostEstimate(
            flops=2 * rows * 256 * (5120 + half), bytes_accessed=8_000_000, transcendentals=0
        ),
    )(tok_mine, tok_other, down, gate, up_half, mine, other)


def tiled(x, width):
    return jnp.concatenate([x] * (width // x.shape[1]), axis=1)


def step(q, cot, keys, values, state, mask):
    wide = (q.shape[0], HEAD_DIM)
    scores = rows_dot(q, keys)
    if mask is not None:
        scores = jnp.where(mask, scores, MASKED)
    top = jnp.broadcast_to(jnp.max(scores, axis=-1, keepdims=True), wide)
    if state is not None:
        top = jnp.maximum(top, state[0])
        fade = jnp.exp2((state[0] - top) * EXP2_SCALE)
    weights = jnp.exp2((scores - tiled(top, scores.shape[1])) * EXP2_SCALE)
    products = weights * rows_dot(cot, values)
    total = jnp.broadcast_to(jnp.sum(weights, axis=-1, keepdims=True), wide)
    delta = jnp.broadcast_to(jnp.sum(products, axis=-1, keepdims=True), wide)
    both = jnp.dot(
        weights.astype(bf16), jnp.concatenate([values, keys], axis=1), preferred_element_type=f32
    )
    acc_v, acc_k = both[:, :HEAD_DIM], both[:, HEAD_DIM:]
    acc_g = jnp.dot(products.astype(bf16), keys, preferred_element_type=f32)
    if state is not None:
        total = total + fade * state[1]
        delta = delta + fade * state[2]
        acc_v = acc_v + fade * state[3]
        acc_k = acc_k + fade * state[4]
        acc_g = acc_g + fade * state[5]
    return top, total, delta, acc_v, acc_k, acc_g


STATES = 6


def attend_body(*refs, kind, reach, heads, first=0):
    refs = list(refs)
    place, _, query, cot_mine, other = refs[:5]
    del refs[:5]
    count = {"own": 2, "far": 4, "edge": 2, "close": 2}[kind]
    pieces = refs[:count]
    del refs[:count]
    state_in = None
    if kind != "own":
        state_in = refs[:STATES]
        del refs[:STATES]
    half = cot_mine.shape[1]
    rows = cot_mine.shape[0]
    both_rows = CORES * rows
    core, z = place[0], place[1]
    unroll = 2 if heads % 2 == 0 else heads

    def columns(h, base=0):
        return pl.ds(pl.multiple_of(h * HEAD_DIM + base, HEAD_DIM), HEAD_DIM)

    def head(h, piece_refs, mask=None):
        at = columns(h + first)
        cot = jnp.concatenate([cot_mine[:, at], other[:, columns(h + first, half)]], axis=0)
        keys = jnp.concatenate([p[:, columns(h)] for p in piece_refs], axis=0)
        values_at = columns(h, heads * HEAD_DIM)
        values = jnp.concatenate([p[:, values_at] for p in piece_refs], axis=0)
        state = None if state_in is None else tuple(s[:, at] for s in state_in)
        return step(query[:, at], cot, keys, values, state, mask)

    if kind in ("own", "far"):
        token_out, state_out = refs[0], refs[1:]
        token_out[...] = jnp.zeros_like(token_out)

        def run(piece_refs, mask=None):
            def one_head(h, carry):
                new = head(h, piece_refs, mask)
                for ref, value in zip(state_out, new, strict=True):
                    ref[:, columns(h)] = value
                return carry

            lax.fori_loop(0, heads, one_head, 0, unroll=unroll)

        if kind == "own":
            shape = (both_rows, both_rows)
            r = lax.broadcasted_iota(jnp.int32, shape, 0)
            s = lax.broadcasted_iota(jnp.int32, shape, 1)
            mine_at, other_at = core * rows, (1 - core) * rows - rows
            row_at = r + jnp.where(r < rows, mine_at, other_at)
            key_at = s + jnp.where(s < rows, mine_at, other_at)
            run(pieces, key_at <= row_at)
            return
        near, wrapped = reach

        @pl.when(z >= wrapped)
        def _():
            run(pieces)

        @pl.when(jnp.logical_and(z >= near, z < wrapped))
        def _():
            run(pieces[:2])

        @pl.when(z < near)
        def _():
            for a, b in zip(state_in, state_out, strict=True):
                b[...] = a[...]

        return

    if kind == "close":
        early, up, low, gates, tok_mine, tok_other = refs[:6]
        del refs[:6]
        att_mine, att_other, grad, dqueries, att, sems = refs
    else:
        att_mine, att_other, dqueries, att, sems = refs

    def outs(at):
        return [
            pltpu.make_async_copy(att.at[pl.ds(0, rows), at], att_mine.at[:, at], sems.at[0]),
            pltpu.make_async_copy(att.at[pl.ds(rows, rows), at], att_other.at[:, at], sems.at[1]),
        ]

    def close(seen):
        def one_head(h, carry):
            at = columns(h)
            state = head(h, pieces) if seen else tuple(s[:, columns(h + first)] for s in state_in)
            _, total, delta, acc_v, acc_k, acc_g = state
            inverse = 1.0 / total
            att[:, at] = (acc_v * inverse).astype(bf16)
            for copy in outs(at):
                copy.start()
            dquery = SCORE_SCALE * (acc_g * inverse - (delta * inverse) * (acc_k * inverse))
            dqueries[:, at] = dquery.astype(bf16)
            return carry

        lax.fori_loop(0, heads, one_head, 0, unroll=unroll)

    seen = z >= reach[0]
    pl.when(seen)(lambda: close(True))
    pl.when(jnp.logical_not(seen))(lambda: close(False))
    if kind == "edge":
        for copy in outs(pl.ds(0, heads * HEAD_DIM)):
            copy.wait()
        return
    split = first * HEAD_DIM
    spread = expert_columns(up.shape[0]).astype(bf16)
    dmixed = rows_dot(early[...], up[:, :split]) + rows_dot(dqueries[...], up[:, split:])
    product = ADAPTER_SCALE * dmixed * low[...].astype(f32)
    dgates = jnp.zeros((EXPERTS, both_rows), f32)
    for _ in range(3):
        part = product.astype(bf16)
        dgates = dgates + rows_dot(spread, part)
        product = product - part.astype(f32)
    g = gates[...]
    dlogits = (g * (dgates - jnp.sum(g * dgates, axis=0, keepdims=True))).astype(bf16)
    width = tok_mine.shape[1]
    chunk = CORES * LANES
    total = jnp.concatenate(
        [
            jnp.dot(
                dlogits,
                jnp.concatenate([tok_mine[:, at : at + chunk], tok_other[:, at : at + chunk]], axis=0),
                preferred_element_type=f32,
            )
            for at in range(0, width, chunk)
        ],
        axis=1,
    )
    per_block = grad.shape[1] // HALF_TILE
    for i in range(grad.shape[0] * per_block):
        t, u = i // 2, i % 2
        b, j = i // per_block, i % per_block
        grad[b, j * HALF_TILE : (j + 1) * HALF_TILE, :] = total[
            u * HALF_TILE : (u + 1) * HALF_TILE, t * LANES : (t + 1) * LANES
        ].astype(bf16)
    for copy in outs(pl.ds(0, heads * HEAD_DIM)):
        copy.wait()


HALF_TILE = EXPERTS // 2
LANES = 128


def gather_blocks_body(blocks, out):
    per_block = blocks.shape[1] // HALF_TILE
    for i in range(blocks.shape[0] * per_block):
        t, u = i // 2, i % 2
        b, j = i // per_block, i % per_block
        out[u * HALF_TILE : (u + 1) * HALF_TILE, t * LANES : (t + 1) * LANES] = blocks[
            b, j * HALF_TILE : (j + 1) * HALF_TILE, :
        ].astype(f32)


def in_vmem(x):
    return pltpu.with_memory_space_constraint(x, pltpu.VMEM)


def attend(kind, reach, place, token, query, cot_mine, other, pieces, state, tail=()):
    both_rows, half = query.shape
    heads = pieces[0].shape[1] // (2 * HEAD_DIM)
    rows = both_rows // CORES
    here = heads * HEAD_DIM
    first = 0
    operands = [place, token, query, cot_mine, other, *pieces, *state, *tail]
    if kind in ("own", "far"):
        out_shape = [jax.ShapeDtypeStruct((8, LANES), f32)]
        out_shape += [pltpu.VMEM((both_rows, half), f32)] * STATES
        out_specs = [WHOLE] * len(out_shape)
        scratch = []
    else:
        out_shape = [pltpu.HBM((rows, here), bf16)] * CORES
        scratch = [pltpu.VMEM((both_rows, here), bf16), pltpu.SemaphoreType.DMA((CORES,))]
        if kind == "edge":
            out_shape += [pltpu.VMEM((both_rows, here), bf16)]
        else:
            first = tail[0].shape[1] // HEAD_DIM
            n, width = lax.axis_size(SEQ), tail[-1].shape[1]
            blocks = (n, EXPERTS * width // n // LANES, LANES)
            out_shape += [jax.ShapeDtypeStruct(blocks, bf16)]
            scratch = [pltpu.VMEM((both_rows, here), bf16)] + scratch
        out_specs = [pl.BlockSpec(memory_space=pl.ANY)] * CORES + [WHOLE]
    keys = sum(p.shape[0] for p in pieces)
    return pl.pallas_call(
        functools.partial(attend_body, kind=kind, reach=reach, heads=heads, first=first),
        in_specs=[SCALAR, pl.BlockSpec(memory_space=pl.ANY)] + [WHOLE] * (len(operands) - 2),
        out_specs=out_specs,
        out_shape=out_shape,
        scratch_shapes=scratch,
        compiler_params=pltpu.CompilerParams(vmem_limit_bytes=VMEM_LIMIT),
        cost_estimate=pl.CostEstimate(
            flops=20 * both_rows * keys * here, bytes_accessed=8_000_000, transcendentals=0
        ),
    )(*operands)


def sent(value, axis, size):
    copies = jnp.broadcast_to(value[None], (size, *value.shape))
    return lax.all_to_all(copies, axis, 0, 0, tiled=True)


def total_of(blocks, shape):
    own = lax.all_to_all(blocks, SEQ, 0, 0, tiled=True).astype(f32).sum(axis=0).astype(bf16)
    own = sent(own, DP, lax.axis_size(DP)).astype(f32).sum(axis=0).astype(bf16)
    whole = in_vmem(sent(own, SEQ, lax.axis_size(SEQ)))
    return pl.pallas_call(
        gather_blocks_body,
        in_specs=[WHOLE],
        out_specs=WHOLE,
        out_shape=jax.ShapeDtypeStruct(shape, f32),
        name="gather_blocks",
    )(whole)


def after(arrays, token):
    *arrays, token = lax.optimization_barrier((*arrays, token))
    return arrays, token


def shards(tokens, base_query, k_base, v_base, cotangent, adapter_down, up_weight, gate_weight):
    width = k_base.shape[2]
    half = width // CORES
    n = lax.axis_size("z")
    core, z = lax.axis_index("c"), lax.axis_index("z")
    place = jnp.stack([core, z]).astype(jnp.int32)
    ahead = [(i, (i + 1) % n) for i in range(n)]
    back = [(i, (i - 1) % n) for i in range(n)]
    swap = [(0, 1), (1, 0)]

    def cross(way):
        return [(2 * i + c, 2 * ((i + way) % n) + 1 - c) for i in range(n) for c in range(2)]

    k_mine, k_other = halve(k_base)
    fa = [moved(k_mine, ahead)]
    kb = [moved(k_other, cross(-1), SEQ)]
    v_mine, v_other = halve(v_base)
    fa = [None, jnp.concatenate([fa[0], moved(v_mine, ahead)], axis=1)]
    v_back = moved(v_other, cross(-1), SEQ)
    kb = [None, jnp.concatenate([kb[0], v_back], axis=1)]
    a0 = jnp.concatenate([k_mine, v_mine], axis=1)
    other_kv = jnp.concatenate([k_other, v_other], axis=1)
    b0 = moved(other_kv, swap, "c")
    fb = [b0, moved(other_kv, cross(1), SEQ)]
    ka = [a0, moved(a0, back)]
    mine_qc, other_qc = pack(base_query, cotangent)
    qc = moved(other_qc, swap, "c")
    tok_mine = tokens[0]
    tok_other = moved(tok_mine, swap, "c")

    up_half = lax.dynamic_slice_in_dim(up_weight, core * half, half, 1)
    query, low, gates, tok_other = make_query(
        tok_mine, tok_other, adapter_down, gate_weight, up_half, mine_qc, qc
    )
    cot_mine = mine_qc[:, half:]
    common = (query, cot_mine, qc)
    fa.append(lax.ppermute(fa[1], "z", ahead))
    kb.append(lax.ppermute(kb[1], "z", back))
    token = jnp.zeros((8, LANES), f32)
    token, *state = attend("own", None, place, token, *common, (a0, b0), ())
    (x, y), token = after((fb[1], ka[1]), token)
    fb.append(lax.ppermute(x, "z", ahead))
    ka.append(lax.ppermute(y, "z", back))
    for d in range(1, n // 2):
        pieces = (fa[d], fb[d], ka[d], kb[d])
        state = [in_vmem(s) for s in state]
        token, *state = attend("far", (d, n - d), place, token, *common, pieces, state)
        if d + 1 < n // 2:
            (x, y), token = after((fa[d + 1], kb[d + 1]), token)
            if d + 2 < n // 2:
                fa.append(lax.ppermute(x, "z", ahead))
                kb.append(lax.ppermute(y, "z", back))
        if d + 2 < n // 2:
            fb.append(moved(fb[d + 1], ahead))
            ka.append(moved(ka[d + 1], back))
    parts = []
    heads = half // HEAD_DIM
    split = heads - max(1, 3 * heads // 10)
    for start, stop in ((0, split), (split, heads)):
        cut = [head_part(p, start, stop) for p in (x, y)]
        parts.append((moved(cut[0], ahead), moved(cut[1], back)))
    common = tuple(in_vmem(v) for v in common)
    state = [in_vmem(v) for v in state]
    reach = (n // 2, n)
    mine_1, other_1, early = attend("edge", reach, place, token, *common, parts[0], state)
    tail = (in_vmem(early), in_vmem(up_half), low, gates, in_vmem(tok_mine), in_vmem(tok_other))
    mine_2, other_2, grad = attend("close", reach, place, token, *common, parts[1], state, tail)
    back_1, back_2 = lax.ppermute(other_1, "c", swap), lax.ppermute(other_2, "c", swap)
    attended = jnp.where(
        core == 0,
        jnp.concatenate([mine_1, mine_2, back_1, back_2], axis=1),
        jnp.concatenate([back_1, back_2, mine_1, mine_2], axis=1),
    )
    return attended[None], total_of(grad, (EXPERTS, tokens.shape[2]))


def moved(value, pairs, axis="z"):
    return lax.ppermute(value, axis, pairs)


def head_part(piece, start, stop):
    half = piece.shape[1] // 2
    a, b = start * HEAD_DIM, stop * HEAD_DIM
    return jnp.concatenate([piece[:, a:b], piece[:, half + a : half + b]], axis=1)


def solution(mesh):
    split = Mesh(mesh.devices.reshape(4, 4, 8, 2), AXES)
    rows = P(DP, SEQ, None)
    return jax.shard_map(
        shards,
        mesh=split,
        in_specs=(rows,) * 5 + (P(),) * 3,
        out_specs=(rows, P()),
        check_vma=False,
    )
```
